16 devices in a mesh: rep: 2 (over y, z), grp: 8 (over x, core).
Axes of the slice: x: 4, y: 2, z: 1, core: 2. Of those that a mesh axis runs over, the one named last changes fastest.
The devices are a block of a 4x4x8 slice.
Arguments:
- x_in: bfloat16 [1024, 4096], P(('rep', 'grp')), parts along dimension 0
- seq_len: int32 [1024], P(('rep', 'grp')), parts along dimension 0
- k_cache: bfloat16 [1024, 512, 2, 128], P(('rep', 'grp')), parts along dimension 0
- v_cache: bfloat16 [1024, 512, 2, 128], P(('rep', 'grp')), parts along dimension 0
- gamma_attn: bfloat16 [4096], replicated
- w_qkv: bfloat16 [4096, 4608], replicated
- b_qkv: bfloat16 [4608], replicated
- w_proj: bfloat16 [4096, 4096], replicated
- gamma_mlp: bfloat16 [4096], replicated
- w_in: bfloat16 [2, 13696, 4096], P(None, 'grp')
- w_out: bfloat16 [13696, 4096], P('grp')
Outputs:
- output 1: bfloat16 [1024, 4096], P(('rep', 'grp')), parts along dimension 0
- output 2: bfloat16 [1024, 512, 2, 128], P(('rep', 'grp')), parts along dimension 0
- output 3: bfloat16 [1024, 512, 2, 128], P(('rep', 'grp')), parts along dimension 0
There are 2 independent parts. The reference program is written for one: setup_inputs(seed, part) draws one part's arguments, and reference() takes and returns one part's arrays. A program takes and returns all parts, laid end to end along the dimension named above; an argument that names none is the same for every part.
All inputs are finite; a program needn't handle non-finite values.
Results may differ from the reference program's by a relative error of at most 0.00892782.
Values are sent between devices in bfloat16 or wider.
A program may use at most 768 MiB of HBM per device.

```python
import jax
import jax.numpy as jnp
from jax import lax

HIDDEN = 4096
HEADS = 32
KV_HEADS = 2
HEAD = 128
FFN = 13696
LMAX = 512
BATCH = 512
ROPE_BASE = 10000
QKV_WIDTH = (HEADS + 2 * KV_HEADS) * HEAD
ROT_DIM = HEAD // 2
EPS = 1e-5


def setup_inputs(seed: int = 0, part: int = 0) -> dict:
    keys = jax.random.split(jax.random.key(seed), 10)
    gamma_attn = (1.0 + 0.3 * jax.random.normal(keys[0], (HIDDEN,), jnp.float32)).astype(jnp.bfloat16)
    w_qkv = (jax.random.normal(keys[1], (HIDDEN, QKV_WIDTH), jnp.float32) * HIDDEN ** -0.5).astype(jnp.bfloat16)
    b_qkv = (0.5 * jax.random.normal(keys[2], (QKV_WIDTH,), jnp.float32)).astype(jnp.bfloat16)
    w_proj = (jax.random.normal(keys[3], (HEADS * HEAD, HIDDEN), jnp.float32) * (HEADS * HEAD) ** -0.5).astype(jnp.bfloat16)
    gamma_mlp = (1.0 + 0.3 * jax.random.normal(keys[4], (HIDDEN,), jnp.float32)).astype(jnp.bfloat16)
    w_in = (jax.random.normal(keys[5], (2, FFN, HIDDEN), jnp.float32) * HIDDEN ** -0.5).astype(jnp.bfloat16)
    w_out = (jax.random.normal(keys[6], (FFN, HIDDEN), jnp.float32) * FFN ** -0.5).astype(jnp.bfloat16)
    x_in = jax.random.normal(jax.random.fold_in(keys[7], part), (BATCH, HIDDEN), jnp.float32).astype(jnp.bfloat16)
    seq_len = jax.random.randint(jax.random.fold_in(keys[8], part), (BATCH,), 1, LMAX, dtype=jnp.int32)
    seq_len = seq_len.at[0].set(LMAX - 1).at[BATCH - 1].set(1)
    cache_keys = jax.random.split(jax.random.fold_in(keys[9], part), 3)
    cache_shape = (BATCH, LMAX, KV_HEADS, HEAD)
    k_cache = (2.0 * jax.random.normal(cache_keys[0], cache_shape, jnp.float32)).astype(jnp.bfloat16)
    drift = jnp.cumsum(jax.random.normal(cache_keys[1], cache_shape, jnp.float32), axis=1) * LMAX ** -0.5
    v_cache = (drift + jax.random.normal(cache_keys[2], cache_shape, jnp.float32)).astype(jnp.bfloat16)
    return {'x_in': x_in, 'seq_len': seq_len, 'k_cache': k_cache, 'v_cache': v_cache,
            'gamma_attn': gamma_attn, 'w_qkv': w_qkv, 'b_qkv': b_qkv, 'w_proj': w_proj,
            'gamma_mlp': gamma_mlp, 'w_in': w_in, 'w_out': w_out}


def rms_norm(vals, gain):
    mean_sq = jnp.mean(vals * vals, axis=-1, keepdims=True)
    return (vals * lax.rsqrt(mean_sq + EPS) * gain.astype(jnp.float32)).astype(jnp.bfloat16)


def rotary(vals, positions):
    inv_freq = ROPE_BASE ** (-jnp.arange(0, ROT_DIM, 2, dtype=jnp.float32) / ROT_DIM)
    angles = positions.astype(jnp.float32)[:, None] * inv_freq[None, :]
    cosine = jnp.cos(angles)[:, None, :]
    sine = jnp.sin(angles)[:, None, :]
    pairs = vals[..., :ROT_DIM].reshape(vals.shape[:-1] + (ROT_DIM // 2, 2))
    even_part = pairs[..., 0]
    odd_part = pairs[..., 1]
    rotated = jnp.stack([even_part * cosine - odd_part * sine, odd_part * cosine + even_part * sine], axis=-1)
    return jnp.concatenate([rotated.reshape(vals.shape[:-1] + (ROT_DIM,)), vals[..., ROT_DIM:]], axis=-1)


def reference(x_in, seq_len, k_cache, v_cache, gamma_attn, w_qkv, b_qkv, w_proj, gamma_mlp, w_in, w_out):
    x_f32 = x_in.astype(jnp.float32)
    normed = rms_norm(x_f32, gamma_attn)
    qkv_proj = jnp.dot(normed, w_qkv, preferred_element_type=jnp.float32) + b_qkv.astype(jnp.float32)
    q_width = HEADS * HEAD
    kv_width = KV_HEADS * HEAD
    query_rot = rotary(qkv_proj[:, :q_width].reshape(BATCH, HEADS, HEAD), seq_len).astype(jnp.bfloat16)
    key_new = rotary(qkv_proj[:, q_width:q_width + kv_width].reshape(BATCH, KV_HEADS, HEAD), seq_len).astype(jnp.bfloat16)
    value_new = qkv_proj[:, q_width + kv_width:].reshape(BATCH, KV_HEADS, HEAD).astype(jnp.bfloat16)
    positions = jnp.arange(LMAX, dtype=jnp.int32)
    at_len = (positions[None, :] == seq_len[:, None])[:, :, None, None]
    k_out = jnp.where(at_len, key_new[:, None], k_cache)
    v_out = jnp.where(at_len, value_new[:, None], v_cache)

    def one_seq(seq_args):
        q_row, k_row, v_row, length = seq_args
        q_grouped = q_row.reshape(KV_HEADS, HEADS // KV_HEADS, HEAD).astype(jnp.float32)
        attn_scores = jnp.einsum('gqd,lgd->gql', q_grouped, k_row.astype(jnp.float32)) * HEAD ** -0.5
        attn_scores = jnp.where((positions <= length)[None, None, :], attn_scores, -jnp.inf)
        attn_probs = jax.nn.softmax(attn_scores, axis=-1).astype(jnp.bfloat16)
        context = jnp.einsum('gql,lgd->gqd', attn_probs.astype(jnp.float32), v_row.astype(jnp.float32))
        return context.reshape(HEADS * HEAD).astype(jnp.bfloat16)

    context = lax.map(one_seq, (query_rot, k_out, v_out, seq_len))
    hidden = x_f32 + jnp.dot(context, w_proj, preferred_element_type=jnp.float32)
    mlp_in = rms_norm(hidden, gamma_mlp)
    gate_up = jnp.dot(mlp_in, w_in.reshape(2 * FFN, HIDDEN).T, preferred_element_type=jnp.float32)
    swiglu = (jax.nn.silu(gate_up[:, :FFN]) * gate_up[:, FFN:]).astype(jnp.bfloat16)
    mlp_out = jnp.dot(swiglu, w_out, preferred_element_type=jnp.float32)
    layer_out = (hidden + mlp_out).astype(jnp.bfloat16)
    return (layer_out, k_out, v_out)
```

```python
import functools

import jax
import jax.numpy as jnp
from jax import lax
from jax.experimental import pallas as pl
from jax.experimental.pallas import tpu as pltpu
from jax.sharding import PartitionSpec as P

HEAD_DIM = 128
ROT_DIM = HEAD_DIM // 2
ROPE_BASE = 10000.0
EPS = 1e-5
F32 = jnp.float32
BF16 = jnp.bfloat16

TN = 512
NW = 4
SG = 4
NS = 8
LAG = 3


def rope_tables(seq_len):
    dim = jnp.arange(HEAD_DIM, dtype=jnp.int32)
    freq = ROPE_BASE ** (-(dim - dim % 2).astype(F32) / ROT_DIM)
    freq = jnp.where(dim < ROT_DIM, freq, 0.0)
    angles = seq_len.astype(F32)[:, None] * freq[None, :]
    sign = jnp.where(dim % 2 == 0, -1.0, 1.0).astype(F32)
    return jnp.cos(angles), jnp.sin(angles) * sign[None, :]


def norm(vals, gain):
    mean_sq = jnp.mean(vals * vals, axis=-1, keepdims=True)
    return (vals * lax.rsqrt(mean_sq + EPS) * gain.astype(F32)).astype(BF16)


def attention_kernel(len_ref, x_ref, cos_ref, sin_ref, ga_ref, b_ref, gm_ref, kc, vc, wq, wp,
                     m_ref, h_ref, ko, vo,
                     wbuf, kbuf, vbuf, nbuf, qh, qs, kn, vn, cb, colpos, wsem, insem, outsem):
    rows = x_ref.shape[0]
    heads = qh.shape[0]
    q_tiles = heads * HEAD_DIM // TN
    p_tiles = wp.shape[1] // TN
    groups = rows // SG
    per_tile = TN // HEAD_DIM
    span = kbuf.shape[2]

    def q_copy(tile):
        slot = lax.rem(tile, NW)
        cols = pl.ds(pl.multiple_of(tile * TN, TN), TN)
        return pltpu.make_async_copy(wq.at[:, cols], wbuf.at[slot], wsem.at[slot])

    def p_copy(tile):
        slot = lax.rem(tile, NW)
        cols = pl.ds(pl.multiple_of(tile * TN, TN), TN)
        return pltpu.make_async_copy(wp.at[:, cols], wbuf.at[slot], wsem.at[slot])

    def cache_in(group):
        slot = lax.rem(group, NS)
        seqs = pl.ds(group * SG, SG)
        return (pltpu.make_async_copy(kc.at[seqs], kbuf.at[slot], insem.at[slot, 0]),
                pltpu.make_async_copy(vc.at[seqs], vbuf.at[slot], insem.at[slot, 1]))

    def cache_out(group):
        slot = lax.rem(group, NS)
        seqs = pl.ds(group * SG, SG)
        return (pltpu.make_async_copy(kbuf.at[slot], ko.at[seqs], outsem.at[slot, 0]),
                pltpu.make_async_copy(vbuf.at[slot], vo.at[seqs], outsem.at[slot, 1]))

    for t in range(NW):
        q_copy(t).start()

    row_id = lax.broadcasted_iota(jnp.int32, (heads, span), 0)
    col_id = lax.broadcasted_iota(jnp.int32, (heads, span), 1)
    kv_of_row = row_id // (heads // 2)
    colpos[...] = jnp.where((col_id & 1) == kv_of_row, col_id >> 1, span)

    nbuf[...] = norm(x_ref[...].astype(F32), ga_ref[...])

    lane = lax.broadcasted_iota(jnp.int32, (rows, HEAD_DIM), 1)
    even = (lane & 1) == 0

    def rope(v):
        swapped = jnp.where(even, pltpu.roll(v, HEAD_DIM - 1, 1), pltpu.roll(v, 1, 1))
        return v * cos_ref[...] + swapped * sin_ref[...]

    def qkv_tile(tile):
        q_copy(tile).wait()
        cols = pl.ds(pl.multiple_of(tile * TN, TN), TN)
        out = jnp.dot(nbuf[...], wbuf[lax.rem(tile, NW)], preferred_element_type=F32)
        return out + b_ref[:, cols].astype(F32)

    def q_step(tile, carry):
        out = qkv_tile(tile)
        for i in range(per_tile):
            qh[tile * per_tile + i] = rope(out[:, i * HEAD_DIM:(i + 1) * HEAD_DIM])

        @pl.when(tile + NW < q_tiles + 1)
        def _():
            q_copy(tile + NW).start()

        @pl.when(tile + NW >= q_tiles + 1)
        def _():
            first = (tile + NW - q_tiles - 1) * 2
            for g in range(2):
                for c in cache_in(first + g):
                    c.start()
        return carry

    lax.fori_loop(0, q_tiles, q_step, 0)
    out = qkv_tile(q_tiles)
    for g in range(2):
        for c in cache_in((NW - 1) * 2 + g):
            c.start()
    for g in range(2):
        kn[g] = rope(out[:, g * HEAD_DIM:(g + 1) * HEAD_DIM])
        vn[g] = out[:, (2 + g) * HEAD_DIM:(3 + g) * HEAD_DIM]
    for hd in range(heads):
        qs[:, hd, :] = qh[hd]

    sub = lax.broadcasted_iota(jnp.int32, (16, HEAD_DIM), 0)
    scale = HEAD_DIM ** -0.5

    def group_step(group, carry):
        slot = lax.rem(group, NS)
        for c in cache_in(group):
            c.wait()
        for j in range(SG):
            seq = group * SG + j
            length = len_ref[seq]
            start = pl.multiple_of((length // 8) * 16, 16)
            here = (sub >> 1) == (length - (length // 8) * 8)
            for buf, new in ((kbuf, kn), (vbuf, vn)):
                pattern = jnp.where((sub & 1) == 0, new[0, pl.ds(seq, 1), :], new[1, pl.ds(seq, 1), :])
                old = buf[slot, j, pl.ds(start, 16), :].astype(F32)
                buf[slot, j, pl.ds(start, 16), :] = jnp.where(here, pattern, old).astype(BF16)
        for c in cache_out(group):
            c.start()
        for j in range(SG):
            seq = group * SG + j
            length = len_ref[seq]
            scores = lax.dot_general(qs[seq].astype(BF16), kbuf[slot, j], (((1,), (1,)), ((), ())),
                                     preferred_element_type=F32) * scale
            scores = jnp.where(colpos[...] <= length, scores, -jnp.inf)
            top = jnp.max(scores, axis=-1, keepdims=True)
            weights = jnp.exp(scores - top)
            total = jnp.sum(weights, axis=-1, keepdims=True)
            probs = (weights / total).astype(BF16)
            cb[seq] = jnp.dot(probs, vbuf[slot, j], preferred_element_type=F32)

        @pl.when(group >= LAG)
        def _():
            for c in cache_out(group - LAG):
                c.wait()

        @pl.when(jnp.logical_and(group >= LAG, group - LAG + NS < groups))
        def _():
            for c in cache_in(group - LAG + NS):
                c.start()

        @pl.when(group >= groups - NW)
        def _():
            p_copy(group - (groups - NW)).start()
        return carry

    lax.fori_loop(0, groups, group_step, 0)
    for hd in range(heads):
        nbuf[:, hd * HEAD_DIM:(hd + 1) * HEAD_DIM] = cb[:, hd, :].astype(BF16)

    def p_step(tile, carry):
        p_copy(tile).wait()
        cols = pl.ds(pl.multiple_of(tile * TN, TN), TN)
        out = jnp.dot(nbuf[...], wbuf[lax.rem(tile, NW)], preferred_element_type=F32)
        h_ref[:, cols] = x_ref[:, cols].astype(F32) + out

        @pl.when(tile + NW < p_tiles)
        def _():
            p_copy(tile + NW).start()
        return carry

    lax.fori_loop(0, p_tiles, p_step, 0)
    m_ref[...] = norm(h_ref[...], gm_ref[...])
    for g in range(LAG):
        for c in cache_out(groups - LAG + g):
            c.wait()


def attention_block(x_in, seq_len, k_cache, v_cache, gamma_attn, w_qkv, b_qkv, w_proj, gamma_mlp):
    rows, width = x_in.shape
    cache_len, kv_heads = k_cache.shape[1], k_cache.shape[2]
    heads = w_proj.shape[0] // HEAD_DIM
    span = cache_len * kv_heads
    cos, sin = rope_tables(seq_len)
    flat = (rows, span, HEAD_DIM)
    vmem = pl.BlockSpec(memory_space=pltpu.VMEM)
    hbm = pl.BlockSpec(memory_space=pl.ANY)
    m, h, k_out, v_out = pl.pallas_call(
        attention_kernel,
        out_shape=(jax.ShapeDtypeStruct((rows, width), BF16), jax.ShapeDtypeStruct((rows, width), F32),
                   jax.ShapeDtypeStruct(flat, BF16), jax.ShapeDtypeStruct(flat, BF16)),
        in_specs=[pl.BlockSpec(memory_space=pltpu.SMEM)] + [vmem] * 6 + [hbm] * 4,
        out_specs=(vmem, vmem, hbm, hbm),
        scratch_shapes=[
            pltpu.VMEM((NW, width, TN), BF16),
            pltpu.VMEM((NS, SG, span, HEAD_DIM), BF16),
            pltpu.VMEM((NS, SG, span, HEAD_DIM), BF16),
            pltpu.VMEM((rows, width), BF16),
            pltpu.VMEM((heads, rows, HEAD_DIM), F32),
            pltpu.VMEM((rows, heads, HEAD_DIM), F32),
            pltpu.VMEM((kv_heads, rows, HEAD_DIM), F32),
            pltpu.VMEM((kv_heads, rows, HEAD_DIM), F32),
            pltpu.VMEM((rows, heads, HEAD_DIM), F32),
            pltpu.VMEM((heads, span), jnp.int32),
            pltpu.SemaphoreType.DMA((NW,)),
            pltpu.SemaphoreType.DMA((NS, 2)),
            pltpu.SemaphoreType.DMA((NS, 2)),
        ],
        compiler_params=pltpu.CompilerParams(vmem_limit_bytes=56 * 1024 * 1024),
        name='attention_block',
    )(seq_len, x_in, cos, sin, gamma_attn[None, :], b_qkv[None, :], gamma_mlp[None, :],
      k_cache.reshape(flat), v_cache.reshape(flat), w_qkv, w_proj)
    return m, h, k_out.reshape(k_cache.shape), v_out.reshape(v_cache.shape)


def solution(mesh):
    row_spec = P(('rep', 'grp'))
    repl_spec = P()

    def local_layer(x_in, seq_len, k_cache, v_cache, gamma_attn, w_qkv, b_qkv, w_proj, gamma_mlp, w_in, w_out):
        mlp_in, hidden, k_out, v_out = attention_block(
            x_in, seq_len, k_cache, v_cache, gamma_attn, w_qkv, b_qkv, w_proj, gamma_mlp)
        group_rows = lax.all_gather(mlp_in, 'grp', axis=0, tiled=True)
        gate_up = jnp.einsum('bh,cfh->bcf', group_rows, w_in, preferred_element_type=jnp.float32)
        swiglu = (jax.nn.silu(gate_up[:, 0]) * gate_up[:, 1]).astype(jnp.bfloat16)
        part_sum = jnp.dot(swiglu, w_out, preferred_element_type=jnp.float32).astype(jnp.bfloat16)
        mlp_out = lax.psum_scatter(part_sum, 'grp', scatter_dimension=0, tiled=True)
        layer_out = (hidden + mlp_out.astype(jnp.float32)).astype(jnp.bfloat16)
        return layer_out, k_out, v_out

    return jax.shard_map(local_layer, mesh=mesh,
                         in_specs=(row_spec, row_spec, row_spec, row_spec, repl_spec, repl_spec, repl_spec,
                                   repl_spec, repl_spec, P(None, 'grp', None), P('grp', None)),
                         out_specs=(row_spec, row_spec, row_spec), check_vma=False)
```

```python
import functools

import jax
import jax.numpy as jnp
from jax import lax
from jax.experimental import pallas as pl
from jax.experimental.pallas import tpu as pltpu
from jax.sharding import PartitionSpec as P

HEAD_DIM = 128
ROT_DIM = HEAD_DIM // 2
ROPE_BASE = 10000.0
EPS = 1e-5
F32 = jnp.float32
BF16 = jnp.bfloat16

TN = 512
NW = 4
SG = 4
NS = 8
LAG = 3


def rope_tables(seq_len):
    dim = jnp.arange(HEAD_DIM, dtype=jnp.int32)
    freq = ROPE_BASE ** (-(dim - dim % 2).astype(F32) / ROT_DIM)
    freq = jnp.where(dim < ROT_DIM, freq, 0.0)
    angles = seq_len.astype(F32)[:, None] * freq[None, :]
    sign = jnp.where(dim % 2 == 0, -1.0, 1.0).astype(F32)
    return jnp.cos(angles), jnp.sin(angles) * sign[None, :]


def norm(vals, gain):
    mean_sq = jnp.mean(vals * vals, axis=-1, keepdims=True)
    return (vals * lax.rsqrt(mean_sq + EPS) * gain.astype(F32)).astype(BF16)


def attention_kernel(len_ref, x_ref, cos_ref, sin_ref, ga_ref, b_ref, gm_ref, kc, vc, wq, wp,
                     m_ref, h_ref, ko, vo,
                     wbuf, kbuf, vbuf, nbuf, qh, qs, kn, vn, cb, colpos, wsem, insem, outsem):
    rows = x_ref.shape[0]
    heads = qh.shape[0]
    q_tiles = heads * HEAD_DIM // TN
    p_tiles = wp.shape[1] // TN
    groups = rows // SG
    per_tile = TN // HEAD_DIM
    span = kbuf.shape[2]

    def q_copy(tile):
        slot = lax.rem(tile, NW)
        cols = pl.ds(pl.multiple_of(tile * TN, TN), TN)
        return pltpu.make_async_copy(wq.at[:, cols], wbuf.at[slot], wsem.at[slot])

    def p_copy(tile):
        slot = lax.rem(tile, NW)
        cols = pl.ds(pl.multiple_of(tile * TN, TN), TN)
        return pltpu.make_async_copy(wp.at[:, cols], wbuf.at[slot], wsem.at[slot])

    def cache_in(group):
        slot = lax.rem(group, NS)
        seqs = pl.ds(group * SG, SG)
        return (pltpu.make_async_copy(kc.at[seqs], kbuf.at[slot], insem.at[slot, 0]),
                pltpu.make_async_copy(vc.at[seqs], vbuf.at[slot], insem.at[slot, 1]))

    def cache_out(group):
        slot = lax.rem(group, NS)
        seqs = pl.ds(group * SG, SG)
        return (pltpu.make_async_copy(kbuf.at[slot], ko.at[seqs], outsem.at[slot, 0]),
                pltpu.make_async_copy(vbuf.at[slot], vo.at[seqs], outsem.at[slot, 1]))

    for t in range(NW):
        q_copy(t).start()

    row_id = lax.broadcasted_iota(jnp.int32, (heads, span), 0)
    col_id = lax.broadcasted_iota(jnp.int32, (heads, span), 1)
    kv_of_row = row_id // (heads // 2)
    colpos[...] = jnp.where((col_id & 1) == kv_of_row, col_id >> 1, span)

    nbuf[...] = norm(x_ref[...].astype(F32), ga_ref[...])

    lane = lax.broadcasted_iota(jnp.int32, (rows, HEAD_DIM), 1)
    even = (lane & 1) == 0

    def rope(v):
        swapped = jnp.where(even, pltpu.roll(v, HEAD_DIM - 1, 1), pltpu.roll(v, 1, 1))
        return v * cos_ref[...] + swapped * sin_ref[...]

    def qkv_tile(tile):
        q_copy(tile).wait()
        cols = pl.ds(pl.multiple_of(tile * TN, TN), TN)
        out = jnp.dot(nbuf[...], wbuf[lax.rem(tile, NW)], preferred_element_type=F32)
        return out + b_ref[:, cols].astype(F32)

    def q_step(tile, carry):
        out = qkv_tile(tile)
        for i in range(per_tile):
            qh[tile * per_tile + i] = rope(out[:, i * HEAD_DIM:(i + 1) * HEAD_DIM])

        @pl.when(tile + NW < q_tiles + 1)
        def _():
            q_copy(tile + NW).start()

        @pl.when(tile + NW >= q_tiles + 1)
        def _():
            first = (tile + NW - q_tiles - 1) * 2
            for g in range(2):
                for c in cache_in(first + g):
                    c.start()
        return carry

    lax.fori_loop(0, q_tiles, q_step, 0)
    out = qkv_tile(q_tiles)
    for g in range(2):
        for c in cache_in((NW - 1) * 2 + g):
            c.start()
    for g in range(2):
        kn[g] = rope(out[:, g * HEAD_DIM:(g + 1) * HEAD_DIM])
        vn[g] = out[:, (2 + g) * HEAD_DIM:(3 + g) * HEAD_DIM]
    for hd in range(heads):
        qs[:, hd, :] = qh[hd]

    sub = lax.broadcasted_iota(jnp.int32, (16, HEAD_DIM), 0)
    scale = HEAD_DIM ** -0.5

    def group_step(group, carry):
        slot = lax.rem(group, NS)
        for c in cache_in(group):
            c.wait()
        for j in range(SG):
            seq = group * SG + j
            length = len_ref[seq]
            start = pl.multiple_of((length // 8) * 16, 16)
            here = (sub >> 1) == (length - (length // 8) * 8)
            for buf, new in ((kbuf, kn), (vbuf, vn)):
                pattern = jnp.where((sub & 1) == 0, new[0, pl.ds(seq, 1), :], new[1, pl.ds(seq, 1), :])
                old = buf[slot, j, pl.ds(start, 16), :].astype(F32)
                buf[slot, j, pl.ds(start, 16), :] = jnp.where(here, pattern, old).astype(BF16)
        for c in cache_out(group):
            c.start()
        for j in range(SG):
            seq = group * SG + j
            length = len_ref[seq]
            scores = lax.dot_general(qs[seq].astype(BF16), kbuf[slot, j], (((1,), (1,)), ((), ())),
                                     preferred_element_type=F32) * scale
            scores = jnp.where(colpos[...] <= length, scores, -jnp.inf)
            top = jnp.max(scores, axis=-1, keepdims=True)
            weights = jnp.exp(scores - top)
            total = jnp.sum(weights, axis=-1, keepdims=True)
            probs = (weights / total).astype(BF16)
            cb[seq] = jnp.dot(probs, vbuf[slot, j], preferred_element_type=F32)

        @pl.when(group >= LAG)
        def _():
            for c in cache_out(group - LAG):
                c.wait()

        @pl.when(jnp.logical_and(group >= LAG, group - LAG + NS < groups))
        def _():
            for c in cache_in(group - LAG + NS):
                c.start()

        @pl.when(group >= groups - NW)
        def _():
            p_copy(group - (groups - NW)).start()
        return carry

    lax.fori_loop(0, groups, group_step, 0)
    for hd in range(heads):
        nbuf[:, hd * HEAD_DIM:(hd + 1) * HEAD_DIM] = cb[:, hd, :].astype(BF16)

    def p_step(tile, carry):
        p_copy(tile).wait()
        cols = pl.ds(pl.multiple_of(tile * TN, TN), TN)
        out = jnp.dot(nbuf[...], wbuf[lax.rem(tile, NW)], preferred_element_type=F32)
        h_ref[:, cols] = x_ref[:, cols].astype(F32) + out

        @pl.when(tile + NW < p_tiles)
        def _():
            p_copy(tile + NW).start()
        return carry

    lax.fori_loop(0, p_tiles, p_step, 0)
    m_ref[...] = norm(h_ref[...], gm_ref[...])
    for g in range(LAG):
        for c in cache_out(groups - LAG + g):
            c.wait()


def attention_block(x_in, seq_len, k_cache, v_cache, gamma_attn, w_qkv, b_qkv, w_proj, gamma_mlp):
    rows, width = x_in.shape
    cache_len, kv_heads = k_cache.shape[1], k_cache.shape[2]
    heads = w_proj.shape[0] // HEAD_DIM
    span = cache_len * kv_heads
    cos, sin = rope_tables(seq_len)
    flat = (rows, span, HEAD_DIM)
    vmem = pl.BlockSpec(memory_space=pltpu.VMEM)
    hbm = pl.BlockSpec(memory_space=pl.ANY)
    m, h, k_out, v_out = pl.pallas_call(
        attention_kernel,
        out_shape=(jax.ShapeDtypeStruct((rows, width), BF16), jax.ShapeDtypeStruct((rows, width), F32),
                   jax.ShapeDtypeStruct(flat, BF16), jax.ShapeDtypeStruct(flat, BF16)),
        in_specs=[pl.BlockSpec(memory_space=pltpu.SMEM)] + [vmem] * 6 + [hbm] * 4,
        out_specs=(vmem, vmem, hbm, hbm),
        scratch_shapes=[
            pltpu.VMEM((NW, width, TN), BF16),
            pltpu.VMEM((NS, SG, span, HEAD_DIM), BF16),
            pltpu.VMEM((NS, SG, span, HEAD_DIM), BF16),
            pltpu.VMEM((rows, width), BF16),
            pltpu.VMEM((heads, rows, HEAD_DIM), F32),
            pltpu.VMEM((rows, heads, HEAD_DIM), F32),
            pltpu.VMEM((kv_heads, rows, HEAD_DIM), F32),
            pltpu.VMEM((kv_heads, rows, HEAD_DIM), F32),
            pltpu.VMEM((rows, heads, HEAD_DIM), F32),
            pltpu.VMEM((heads, span), jnp.int32),
            pltpu.SemaphoreType.DMA((NW,)),
            pltpu.SemaphoreType.DMA((NS, 2)),
            pltpu.SemaphoreType.DMA((NS, 2)),
        ],
        compiler_params=pltpu.CompilerParams(vmem_limit_bytes=56 * 1024 * 1024),
        name='attention_block',
    )(seq_len, x_in, cos, sin, gamma_attn[None, :], b_qkv[None, :], gamma_mlp[None, :],
      k_cache.reshape(flat), v_cache.reshape(flat), w_qkv, w_proj)
    return m, h, k_out.reshape(k_cache.shape), v_out.reshape(v_cache.shape)

FT = 1024
HT = 256


def mlp_kernel(m_in, h_in, wi, wo, out_ref,
               rows_all, wib, wob, gbuf, facc, hold, acc, topart, frompart, outbox, from_l, from_r, mid_l, mid_r,
               wsem, isem, gsend, grecv, psend, precv, bsend, brecv):
    me = lax.axis_index('grp')
    chips = lax.axis_size('grp') // 2
    chip, core = me // 2, me % 2
    right = lax.rem(chip + 1, chips) * 2 + core
    left = lax.rem(chip + chips - 1, chips) * 2 + core
    partner = chip * 2 + 1 - core
    r = m_in.shape[0]
    s, g, br = r // 2, 2 * r, 4 * r
    hidden = wo.shape[0]
    full = hidden // HT
    rest = hidden - full * HT
    hpad = wob.shape[0]
    tiles = wo.shape[1] // FT

    def w_copy(j):
        part = pl.ds(pl.multiple_of(j * HT, HT), HT)
        return pltpu.make_async_copy(wi.at[:, part], wib.at[:, part], wsem.at[j])

    last_in = pltpu.make_async_copy(wi.at[:, pl.ds(full * HT, rest)], wib.at[:, pl.ds(full * HT, rest)], wsem.at[full])
    m_copy = pltpu.make_async_copy(m_in, rows_all.at[pl.ds(0, r)], isem.at[0])
    h_copy = pltpu.make_async_copy(h_in, acc, isem.at[1])
    o_copy = pltpu.make_async_copy(wo, wob.at[pl.ds(0, hidden)], isem.at[2])
    m_copy.start()
    for j in range(full):
        w_copy(j).start()
    last_in.start()
    o_copy.start()
    h_copy.start()

    barrier = pltpu.get_barrier_semaphore()
    for dev in (right, left, partner):
        pl.semaphore_signal(barrier, inc=1, device_id={'grp': dev}, device_id_type=pl.DeviceIdType.MESH)
    pl.semaphore_wait(barrier, 3)

    def remote(src, dst, send, recv, dev):
        return pltpu.make_async_remote_copy(src_ref=src, dst_ref=dst, send_sem=send, recv_sem=recv,
                                            device_id={'grp': dev}, device_id_type=pl.DeviceIdType.MESH)

    def gather(n, src, dst, count, dev):
        return remote(rows_all.at[pl.ds(src, count)], rows_all.at[pl.ds(dst, count)], gsend.at[n], grecv.at[n], dev)

    to_r0 = gather(0, 0, r, s, right)
    to_l1 = gather(1, s, r + s, s, left)
    to_r1 = gather(2, s, br + r, s, right)
    to_l0 = gather(3, 0, br + r + s, s, left)
    to_p = gather(4, 0, g, r, partner)
    on_r = gather(5, r, br, s, right)
    on_l = gather(6, r + s, br + s, s, left)
    p_l0 = gather(7, r, g + r, s, partner)
    p_r1 = gather(8, r + s, g + r + s, s, partner)
    p_l1 = gather(9, br + r, br + g + r, s, partner)
    p_r0 = gather(10, br + r + s, br + g + r + s, s, partner)
    p_o0 = gather(11, br, br + g, s, partner)
    p_o1 = gather(12, br + s, br + g + s, s, partner)
    gathers = [to_r0, to_l1, to_r1, to_l0, to_p, on_r, on_l, p_l0, p_r1, p_l1, p_r0, p_o0, p_o1]

    m_copy.wait()
    for c in (to_r0, to_l1, to_p, to_r1, to_l0):
        c.start()
    if hpad > hidden:
        wib[:, hidden:, :] = jnp.zeros((2, hpad - hidden, wib.shape[2]), BF16)
        wob[hidden:, :] = jnp.zeros((hpad - hidden, wob.shape[1]), BF16)

    to_r0.wait_recv()
    on_r.start()
    p_l0.start()
    to_l1.wait_recv()
    on_l.start()
    p_r1.start()
    for c in (to_p, p_l0, p_r1):
        c.wait_recv()

    def gate_tile(blk, j):
        part = pl.ds(pl.multiple_of(j * HT, HT), HT)
        x = rows_all[pl.ds(blk * br, br)]
        dims = (((1,), (1,)), ((), ()))
        gate = lax.dot_general(x, wib[0, part, :], dims, preferred_element_type=F32)
        up = lax.dot_general(x, wib[1, part, :], dims, preferred_element_type=F32)
        gbuf[:, part] = (jax.nn.silu(gate) * up).astype(BF16)

    def cols(t):
        return slice(t * FT, (t + 1) * FT)

    def to_partner(blk, t):
        return remote(topart.at[t], frompart.at[blk, t], psend.at[blk, t], precv.at[blk, t], partner)

    def out_copy(kind, t):
        dst = (from_r.at[0, t], from_l.at[1, t], mid_l.at[t], mid_r.at[t], from_l.at[0, t], from_r.at[1, t])[kind]
        dev = (left, right, right, left, right, left)[kind]
        return remote(outbox.at[kind, t], dst, bsend.at[kind, t], brecv.at[kind, t], dev)

    def post(kind, t, vals):
        outbox[kind, t] = vals.astype(BF16)
        out_copy(kind, t).start()

    def down_tile(blk, t):
        f = jnp.dot(gbuf[...], wob[:, cols(t)], preferred_element_type=F32)
        if blk == 1:
            to_partner(0, t).wait_send()
        topart[t] = f[g:].astype(BF16)
        to_partner(blk, t).start()
        facc[t % 2] = f[:g]

    def finish(blk, t):
        to_partner(blk, t).wait_recv()
        total = facc[t % 2] + frompart[blk, t].astype(F32)
        if blk == 0:
            acc[:, cols(t)] += total[:r]
            post(0, t, total[r:r + s])
            post(1, t, total[r + s:])
        else:
            post(2, t, total[:s])
            post(3, t, total[s:r])
            hold[t] = total[r:]

    def step0(j, carry):
        w_copy(j).wait()
        gate_tile(0, j)
        return carry

    lax.fori_loop(0, full, step0, 0)
    if rest:
        last_in.wait()
        gate_tile(0, full)
    to_r1.wait_recv()
    p_l1.start()
    to_l0.wait_recv()
    p_r0.start()
    o_copy.wait()
    h_copy.wait()
    for t in range(tiles):
        down_tile(0, t)
        if t:
            finish(0, t - 1)
        if t == tiles - 2:
            on_r.wait_recv()
            p_o0.start()
            on_l.wait_recv()
            p_o1.start()
    for c in (p_l1, p_r0, p_o0, p_o1):
        c.wait_recv()

    gate_tile(1, 0)
    finish(0, tiles - 1)

    def step1(j, carry):
        gate_tile(1, j)
        return carry

    lax.fori_loop(1, hpad // HT, step1, 0)
    for t in range(tiles):
        down_tile(1, t)
        if t:
            finish(1, t - 1)
    finish(1, tiles - 1)
    for t in range(tiles):
        out_copy(2, t).wait_recv()
        post(4, t, hold[t, s:] + mid_l[t].astype(F32))
        out_copy(3, t).wait_recv()
        post(5, t, hold[t, :s] + mid_r[t].astype(F32))
    for t in range(tiles):
        for kind in (0, 1, 4, 5):
            out_copy(kind, t).wait_recv()
        for half in range(2):
            part = slice(half * s, (half + 1) * s)
            total = acc[part, cols(t)] + (from_l[half, t].astype(F32) + from_r[half, t].astype(F32))
            out_ref[part, cols(t)] = total.astype(BF16)
    for c in gathers:
        c.wait_send()
    for t in range(tiles):
        to_partner(1, t).wait_send()
        for kind in range(6):
            out_copy(kind, t).wait_send()


def mlp_block(m, h, w_in, w_out):
    rows, width = m.shape
    hidden = w_out.shape[0]
    hpad = -(-hidden // HT) * HT
    tiles = width // FT
    half, group, block = rows // 2, 2 * rows, 4 * rows
    hbm = pl.BlockSpec(memory_space=pl.ANY)
    dma = pltpu.SemaphoreType.DMA
    return pl.pallas_call(
        mlp_kernel,
        out_shape=jax.ShapeDtypeStruct((rows, width), BF16),
        in_specs=[hbm] * 4,
        out_specs=pl.BlockSpec(memory_space=pltpu.VMEM),
        scratch_shapes=[
            pltpu.VMEM((2 * block, width), BF16),
            pltpu.VMEM((2, hpad, width), BF16),
            pltpu.VMEM((hpad, width), BF16),
            pltpu.VMEM((block, hpad), BF16),
            pltpu.VMEM((2, group, FT), F32),
            pltpu.VMEM((tiles, rows, FT), F32),
            pltpu.VMEM((rows, width), F32),
            pltpu.VMEM((tiles, group, FT), BF16),
            pltpu.VMEM((2, tiles, group, FT), BF16),
            pltpu.VMEM((6, tiles, half, FT), BF16),
            pltpu.VMEM((2, tiles, half, FT), BF16),
            pltpu.VMEM((2, tiles, half, FT), BF16),
            pltpu.VMEM((tiles, half, FT), BF16),
            pltpu.VMEM((tiles, half, FT), BF16),
            dma((hpad // HT,)), dma((3,)), dma((13,)), dma((13,)),
            dma((2, tiles)), dma((2, tiles)), dma((6, tiles)), dma((6, tiles)),
        ],
        compiler_params=pltpu.CompilerParams(vmem_limit_bytes=67043328, collective_id=0, has_side_effects=True),
        name='mlp_block',
    )(m, h, w_in, w_out)


def solution(mesh):
    row_spec = P(('rep', 'grp'))
    repl_spec = P()

    def local_layer(x_in, seq_len, k_cache, v_cache, gamma_attn, w_qkv, b_qkv, w_proj, gamma_mlp, w_in, w_out):
        mlp_in, hidden, k_out, v_out = attention_block(
            x_in, seq_len, k_cache, v_cache, gamma_attn, w_qkv, b_qkv, w_proj, gamma_mlp)
        layer_out = mlp_block(mlp_in, hidden, w_in, w_out)
        return layer_out, k_out, v_out

    return jax.shard_map(local_layer, mesh=mesh,
                         in_specs=(row_spec, row_spec, row_spec, row_spec, repl_spec, repl_spec, repl_spec,
                                   repl_spec, repl_spec, P(None, 'grp', None), P('grp', None)),
                         out_specs=(row_spec, row_spec, row_spec), check_vma=False)
```

```python
import math

import jax
import jax.numpy as jnp
from jax import lax
from jax.experimental import pallas as pl
from jax.experimental.pallas import tpu as pltpu
from jax.sharding import PartitionSpec as P

HEAD_DIM = 128
ROT_DIM = HEAD_DIM // 2
ROPE_BASE = 10000.0
EPS = 1e-5
F32 = jnp.float32
BF16 = jnp.bfloat16

TN = 512
NW = 4
SG = 4
NS = 8
LAG = 3


def norm(vals, gain):
    mean_sq = jnp.mean(vals * vals, axis=-1, keepdims=True)
    return (vals * lax.rsqrt(mean_sq + EPS) * gain.astype(F32)).astype(BF16)


def attention_kernel(len_ref, x_ref, ga_ref, b_ref, kc, vc, wq,
                     ctx_ref, ko, vo,
                     wbuf, kbuf, vbuf, nbuf, bias, cos, sin, qh, qs, kn, vn, cb, colpos, wsem, insem, outsem):
    rows = x_ref.shape[0]
    heads = qh.shape[0]
    q_tiles = heads * HEAD_DIM // TN
    groups = rows // SG
    per_tile = TN // HEAD_DIM
    span = kbuf.shape[2]

    def q_copy(tile):
        slot = lax.rem(tile, NW)
        cols = pl.ds(pl.multiple_of(tile * TN, TN), TN)
        return pltpu.make_async_copy(wq.at[:, cols], wbuf.at[slot], wsem.at[slot])

    def cache_in(group):
        slot = lax.rem(group, NS)
        seqs = pl.ds(group * SG, SG)
        return (pltpu.make_async_copy(kc.at[seqs], kbuf.at[slot], insem.at[slot, 0]),
                pltpu.make_async_copy(vc.at[seqs], vbuf.at[slot], insem.at[slot, 1]))

    def cache_out(group):
        slot = lax.rem(group, NS)
        seqs = pl.ds(group * SG, SG)
        return (pltpu.make_async_copy(kbuf.at[slot], ko.at[seqs], outsem.at[slot, 0]),
                pltpu.make_async_copy(vbuf.at[slot], vo.at[seqs], outsem.at[slot, 1]))

    for t in range(NW):
        q_copy(t).start()

    row_id = lax.broadcasted_iota(jnp.int32, (heads, span), 0)
    col_id = lax.broadcasted_iota(jnp.int32, (heads, span), 1)
    kv_of_row = row_id // (heads // 2)
    colpos[...] = jnp.where((col_id & 1) == kv_of_row, col_id >> 1, span)

    nbuf[...] = norm(x_ref[...].astype(F32), ga_ref[...].astype(F32)[None, :])
    bias[...] = b_ref[...].astype(F32)[None, :]
    dim = lax.broadcasted_iota(jnp.int32, (1, HEAD_DIM), 1)
    freq = jnp.exp((dim - (dim & 1)).astype(F32) * (-math.log(ROPE_BASE) / ROT_DIM))
    freq = jnp.where(dim < ROT_DIM, freq, 0.0)
    for i in range(rows):
        cos[i:i + 1, :] = len_ref[i].astype(F32) * freq
    angles = cos[...]
    sign = jnp.where((dim & 1) == 0, -1.0, 1.0)
    cos[...] = jnp.cos(angles)
    sin[...] = jnp.sin(angles) * sign

    lane = lax.broadcasted_iota(jnp.int32, (rows, HEAD_DIM), 1)
    even = (lane & 1) == 0

    def rope(v):
        swapped = jnp.where(even, pltpu.roll(v, HEAD_DIM - 1, 1), pltpu.roll(v, 1, 1))
        return v * cos[...] + swapped * sin[...]

    def qkv_tile(tile):
        q_copy(tile).wait()
        cols = pl.ds(pl.multiple_of(tile * TN, TN), TN)
        out = jnp.dot(nbuf[...], wbuf[lax.rem(tile, NW)], preferred_element_type=F32)
        return out + bias[:, cols]

    def q_step(tile, carry):
        out = qkv_tile(tile)
        for i in range(per_tile):
            qh[tile * per_tile + i] = rope(out[:, i * HEAD_DIM:(i + 1) * HEAD_DIM])

        @pl.when(tile + NW < q_tiles + 1)
        def _():
            q_copy(tile + NW).start()

        @pl.when(tile + NW >= q_tiles + 1)
        def _():
            first = (tile + NW - q_tiles - 1) * 2
            for g in range(2):
                for c in cache_in(first + g):
                    c.start()
        return carry

    lax.fori_loop(0, q_tiles, q_step, 0)
    out = qkv_tile(q_tiles)
    for g in range(2):
        for c in cache_in((NW - 1) * 2 + g):
            c.start()
    for g in range(2):
        kn[g] = rope(out[:, g * HEAD_DIM:(g + 1) * HEAD_DIM])
        vn[g] = out[:, (2 + g) * HEAD_DIM:(3 + g) * HEAD_DIM]
    for hd in range(heads):
        qs[:, hd, :] = qh[hd]

    sub = lax.broadcasted_iota(jnp.int32, (16, HEAD_DIM), 0)
    scale = HEAD_DIM ** -0.5

    def group_step(group, carry):
        slot = lax.rem(group, NS)
        for c in cache_in(group):
            c.wait()
        for j in range(SG):
            seq = group * SG + j
            length = len_ref[seq]
            start = pl.multiple_of((length // 8) * 16, 16)
            here = (sub >> 1) == (length - (length // 8) * 8)
            for buf, new in ((kbuf, kn), (vbuf, vn)):
                pattern = jnp.where((sub & 1) == 0, new[0, pl.ds(seq, 1), :], new[1, pl.ds(seq, 1), :])
                old = buf[slot, j, pl.ds(start, 16), :].astype(F32)
                buf[slot, j, pl.ds(start, 16), :] = jnp.where(here, pattern, old).astype(BF16)
        for c in cache_out(group):
            c.start()
        dims = (((1,), (1,)), ((), ()))
        seqs = [group * SG + j for j in range(SG)]
        scores = [lax.dot_general(qs[seqs[j]].astype(BF16), kbuf[slot, j], dims, preferred_element_type=F32) * scale
                  for j in range(SG)]
        scores = [jnp.where(colpos[...] <= len_ref[seqs[j]], scores[j], -jnp.inf) for j in range(SG)]
        tops = [jnp.max(v, axis=-1, keepdims=True) for v in scores]
        weights = [jnp.exp(v - t) for v, t in zip(scores, tops)]
        totals = [jnp.sum(v, axis=-1, keepdims=True) for v in weights]
        probs = [(v / t).astype(BF16) for v, t in zip(weights, totals)]
        for j in range(SG):
            cb[seqs[j]] = jnp.dot(probs[j], vbuf[slot, j], preferred_element_type=F32)

        @pl.when(group >= LAG)
        def _():
            for c in cache_out(group - LAG):
                c.wait()

        @pl.when(jnp.logical_and(group >= LAG, group - LAG + NS < groups))
        def _():
            for c in cache_in(group - LAG + NS):
                c.start()

        return carry

    lax.fori_loop(0, groups, group_step, 0)
    for hd in range(heads):
        ctx_ref[:, hd * HEAD_DIM:(hd + 1) * HEAD_DIM] = cb[:, hd, :].astype(BF16)
    for g in range(LAG):
        for c in cache_out(groups - LAG + g):
            c.wait()


def attention_block(x_in, seq_len, k_cache, v_cache, gamma_attn, w_qkv, b_qkv):
    rows, width = x_in.shape
    cache_len, kv_heads = k_cache.shape[1], k_cache.shape[2]
    q_width = w_qkv.shape[1] - 2 * kv_heads * HEAD_DIM
    heads = q_width // HEAD_DIM
    span = cache_len * kv_heads
    flat = (rows, span, HEAD_DIM)
    vmem = pl.BlockSpec(memory_space=pltpu.VMEM)
    hbm = pl.BlockSpec(memory_space=pl.ANY)
    ctx, k_out, v_out = pl.pallas_call(
        attention_kernel,
        out_shape=(jax.ShapeDtypeStruct((rows, q_width), BF16),
                   jax.ShapeDtypeStruct(flat, BF16), jax.ShapeDtypeStruct(flat, BF16)),
        in_specs=[pl.BlockSpec(memory_space=pltpu.SMEM)] + [vmem] * 3 + [hbm] * 3,
        out_specs=(vmem, hbm, hbm),
        scratch_shapes=[
            pltpu.VMEM((NW, width, TN), BF16),
            pltpu.VMEM((NS, SG, span, HEAD_DIM), BF16),
            pltpu.VMEM((NS, SG, span, HEAD_DIM), BF16),
            pltpu.VMEM((rows, width), BF16),
            pltpu.VMEM((1, w_qkv.shape[1]), F32),
            pltpu.VMEM((rows, HEAD_DIM), F32),
            pltpu.VMEM((rows, HEAD_DIM), F32),
            pltpu.VMEM((heads, rows, HEAD_DIM), F32),
            pltpu.VMEM((rows, heads, HEAD_DIM), F32),
            pltpu.VMEM((kv_heads, rows, HEAD_DIM), F32),
            pltpu.VMEM((kv_heads, rows, HEAD_DIM), F32),
            pltpu.VMEM((rows, heads, HEAD_DIM), F32),
            pltpu.VMEM((heads, span), jnp.int32),
            pltpu.SemaphoreType.DMA((NW,)),
            pltpu.SemaphoreType.DMA((NS, 2)),
            pltpu.SemaphoreType.DMA((NS, 2)),
        ],
        compiler_params=pltpu.CompilerParams(vmem_limit_bytes=56 * 1024 * 1024),
        name='attention_block',
    )(seq_len, x_in, gamma_attn, b_qkv, k_cache.reshape(flat), v_cache.reshape(flat), w_qkv)
    return ctx, k_out.reshape(k_cache.shape), v_out.reshape(v_cache.shape)


FT = 1024
HT = 256
RELAY_AT = 5


PT = 512
PSLOTS = 6
SHIFT = 2.0 ** 64


def mlp_kernel(ctx_in, x_in, gm_in, wp, wi, wo, out_ref,
               gs, rows_all, rs_all, wib, wob, gbuf, facc, hold, acc, topart, frompart, outbox,
               from_l, from_r, mid_l, mid_r,
               psem, wsem, osem, gsend, grecv, psend, precv, bsend, brecv):
    me = lax.axis_index('grp')
    chips = lax.axis_size('grp') // 2
    chip, core = me // 2, me % 2
    right = lax.rem(chip + 1, chips) * 2 + core
    left = lax.rem(chip + chips - 1, chips) * 2 + core
    partner = chip * 2 + 1 - core
    r = x_in.shape[0]
    s, g, br = r // 2, 2 * r, 4 * r
    hidden = wo.shape[0]
    full = hidden // HT
    rest = hidden - full * HT
    hpad = wob.shape[0]
    tiles = wo.shape[1] // FT

    def w_copy(j):
        part = pl.ds(pl.multiple_of(j * HT, HT), HT)
        return pltpu.make_async_copy(wi.at[:, part], wib.at[:, part], wsem.at[j])

    last_in = pltpu.make_async_copy(wi.at[:, pl.ds(full * HT, rest)], wib.at[:, pl.ds(full * HT, rest)], wsem.at[full])
    o_copy = pltpu.make_async_copy(wo, wob.at[pl.ds(0, hidden)], osem)
    p_tiles = wp.shape[1] // PT
    depth = wp.shape[0] // PT

    def p_part(t, k):
        slot = t % PSLOTS
        buf, row = (wob, slot * PT) if slot < PSLOTS // 2 else (wib.at[1], (slot - PSLOTS // 2) * PT)
        return buf.at[pl.ds(row, PT), pl.ds(k * PT, PT)]

    def p_copy(t, k):
        return pltpu.make_async_copy(wp.at[pl.ds(k * PT, PT), pl.ds(t * PT, PT)], p_part(t, k), psem.at[t % PSLOTS, k])

    for t in range(PSLOTS):
        for k in range(depth):
            p_copy(t, k).start()
    gs[...] = gm_in[...].astype(F32)[None, :] * (1.0 / SHIFT)

    barrier = pltpu.get_barrier_semaphore()
    for dev in (right, left, partner):
        pl.semaphore_signal(barrier, inc=1, device_id={'grp': dev}, device_id_type=pl.DeviceIdType.MESH)
    pl.semaphore_wait(barrier, 3)

    def remote(src, dst, send, recv, dev):
        return pltpu.make_async_remote_copy(src_ref=src, dst_ref=dst, send_sem=send, recv_sem=recv,
                                            device_id={'grp': dev}, device_id_type=pl.DeviceIdType.MESH)

    def gather(n, src, dst, count, dev):
        def at(c):
            def view(first):
                if c == tiles:
                    return rs_all.at[pl.ds(first, count)]
                return rows_all.at[pl.ds(first, count), pl.ds(c * FT, FT)]
            return remote(view(src), view(dst), gsend.at[n, c], grecv.at[n, c], dev)
        return at

    to_r0 = gather(0, 0, r, s, right)
    to_l1 = gather(1, s, r + s, s, left)
    to_r1 = gather(2, s, br + r, s, right)
    to_l0 = gather(3, 0, br + r + s, s, left)
    to_p = gather(4, 0, g, r, partner)
    on_r = gather(5, r, br, s, right)
    on_l = gather(6, r + s, br + s, s, left)
    p_l0 = gather(7, r, g + r, s, partner)
    p_r1 = gather(8, r + s, g + r + s, s, partner)
    p_l1 = gather(9, br + r, br + g + r, s, partner)
    p_r0 = gather(10, br + r + s, br + g + r + s, s, partner)
    p_o0 = gather(11, br, br + g, s, partner)
    p_o1 = gather(12, br + s, br + g + s, s, partner)
    gathers = [to_r0, to_l1, to_r1, to_l0, to_p, on_r, on_l, p_l0, p_r1, p_l1, p_r0, p_o0, p_o1]

    def give(c):
        for copy in (to_r0, to_l1, to_r1, to_l0, to_p):
            copy(c).start()

    def pass_on(c):
        to_r0(c).wait_recv()
        on_r(c).start()
        p_l0(c).start()
        to_l1(c).wait_recv()
        on_l(c).start()
        p_r1(c).start()
        to_r1(c).wait_recv()
        p_l1(c).start()
        to_l0(c).wait_recv()
        p_r0(c).start()

    def pass_far(c):
        on_r(c).wait_recv()
        p_o0(c).start()
        on_l(c).wait_recv()
        p_o1(c).start()

    if hpad > hidden:
        wib[:, hidden:, :] = jnp.zeros((2, hpad - hidden, wib.shape[2]), BF16)
        wob[hidden:, :] = jnp.zeros((hpad - hidden, wob.shape[1]), BF16)

    square = jnp.zeros((r, HEAD_DIM), F32)
    per = FT // PT
    for t in range(p_tiles):
        part = slice(t * PT, (t + 1) * PT)
        out = None
        for k in range(depth):
            p_copy(t, k).wait()
        for k in range(depth):
            term = jnp.dot(ctx_in[:, k * PT:(k + 1) * PT], p_part(t, k)[...], preferred_element_type=F32)
            out = term if out is None else out + term
        hid = x_in[:, part].astype(F32) + out
        acc[:, part] = hid
        rows_all[0:r, part] = (hid * gs[:, part]).astype(BF16)
        for k in range(PT // HEAD_DIM):
            lanes = hid[:, k * HEAD_DIM:(k + 1) * HEAD_DIM]
            square = square + lanes * lanes
        if t + PSLOTS < p_tiles:
            for k in range(depth):
                p_copy(t + PSLOTS, k).start()
        if t == PSLOTS - 1:
            for j in range(full):
                w_copy(j).start()
            if rest:
                last_in.start()
        if t % per == per - 1:
            give(t // per)
        if t == p_tiles - 3:
            pass_on(0)
    o_copy.start()
    mean_sq = jnp.sum(square, axis=-1, keepdims=True) / wp.shape[1]
    rs_all[0:r, :] = jnp.broadcast_to(lax.rsqrt(mean_sq + EPS) * SHIFT, (r, HEAD_DIM))
    give(tiles)
    for c in range(1, tiles + 1):
        pass_on(c)
        pass_far(c - 1)
    pass_far(tiles)
    for c in range(tiles + 1):
        for copy in (to_p, p_l0, p_r1, p_l1, p_r0, p_o0, p_o1):
            copy(c).wait_recv()

    def gate_tile(blk, j):
        part = pl.ds(pl.multiple_of(j * HT, HT), HT)
        x = rows_all[pl.ds(blk * br, br)]
        dims = (((1,), (1,)), ((), ()))
        gate = lax.dot_general(x, wib[0, part, :], dims, preferred_element_type=F32)
        up = lax.dot_general(x, wib[1, part, :], dims, preferred_element_type=F32)
        scale = rs_all[pl.ds(blk * br, br), 0:1]
        gate = jnp.where(scale > 0.0, gate * scale, 0.0)
        up = jnp.where(scale > 0.0, up * scale, 0.0)
        gbuf[:, part] = (jax.nn.silu(gate) * up).astype(BF16)

    def cols(t):
        return slice(t * FT, (t + 1) * FT)

    def to_partner(blk, t):
        return remote(topart.at[t], frompart.at[blk, t], psend.at[blk, t], precv.at[blk, t], partner)

    def out_copy(kind, t):
        dst = (from_r.at[0, t], from_l.at[1, t], mid_l.at[t], mid_r.at[t], from_l.at[0, t], from_r.at[1, t])[kind]
        dev = (left, right, right, left, right, left)[kind]
        return remote(outbox.at[kind, t], dst, bsend.at[kind, t], brecv.at[kind, t], dev)

    def post(kind, t, vals):
        outbox[kind, t] = vals.astype(BF16)
        out_copy(kind, t).start()

    def down_tile(blk, t):
        f = jnp.dot(gbuf[...], wob[:, cols(t)], preferred_element_type=F32)
        if blk == 0:
            to_partner(1, t).wait_send()
        topart[t] = f[g:].astype(BF16)
        to_partner(blk, t).start()
        facc[t % 2] = f[:g]

    def finish(blk, t):
        to_partner(blk, t).wait_recv()
        total = facc[t % 2] + frompart[blk, t].astype(F32)
        if blk == 0:
            acc[:, cols(t)] += total[:r]
            post(0, t, total[r:r + s])
            post(1, t, total[r + s:])
        else:
            post(2, t, total[:s])
            post(3, t, total[s:r])
            hold[t] = total[r:]

    def far_step(j, carry):
        w_copy(j).wait()
        gate_tile(1, j)
        return carry

    def near_step(j, carry):
        gate_tile(0, j)
        return carry

    lax.fori_loop(0, full, far_step, 0)
    if rest:
        last_in.wait()
        gate_tile(1, full)
    o_copy.wait()
    for t in range(tiles):
        down_tile(1, t)
        if t:
            finish(1, t - 1)
    gate_tile(0, 0)
    finish(1, tiles - 1)
    lax.fori_loop(1, RELAY_AT, near_step, 0)
    for t in range(tiles):
        out_copy(2, t).wait_recv()
        post(4, t, hold[t, s:] + mid_l[t].astype(F32))
        out_copy(3, t).wait_recv()
        post(5, t, hold[t, :s] + mid_r[t].astype(F32))
    lax.fori_loop(RELAY_AT, hpad // HT, near_step, 0)
    for t in range(tiles):
        down_tile(0, t)
        if t:
            finish(0, t - 1)
    finish(0, tiles - 1)
    for t in range(tiles):
        for kind in (0, 1, 4, 5):
            out_copy(kind, t).wait_recv()
        for half in range(2):
            part = slice(half * s, (half + 1) * s)
            total = acc[part, cols(t)] + (from_l[half, t].astype(F32) + from_r[half, t].astype(F32))
            out_ref[part, cols(t)] = total.astype(BF16)
    for copy in gathers:
        for c in range(tiles + 1):
            copy(c).wait_send()
    for t in range(tiles):
        to_partner(0, t).wait_send()
        for kind in range(6):
            out_copy(kind, t).wait_send()


def mlp_block(ctx, x_in, gamma_mlp, w_proj, w_in, w_out):
    rows, width = x_in.shape
    hidden = w_out.shape[0]
    hpad = -(-hidden // HT) * HT
    tiles = width // FT
    half, group, block = rows // 2, 2 * rows, 4 * rows
    hbm = pl.BlockSpec(memory_space=pl.ANY)
    vmem = pl.BlockSpec(memory_space=pltpu.VMEM)
    dma = pltpu.SemaphoreType.DMA
    return pl.pallas_call(
        mlp_kernel,
        out_shape=jax.ShapeDtypeStruct((rows, width), BF16),
        in_specs=[vmem] * 3 + [hbm] * 3,
        out_specs=vmem,
        scratch_shapes=[
            pltpu.VMEM((1, width), F32),
            pltpu.VMEM((2 * block, width), BF16),
            pltpu.VMEM((2 * block, HEAD_DIM), F32),
            pltpu.VMEM((2, hpad, width), BF16),
            pltpu.VMEM((hpad, width), BF16),
            pltpu.VMEM((block, hpad), BF16),
            pltpu.VMEM((2, group, FT), F32),
            pltpu.VMEM((tiles, rows, FT), F32),
            pltpu.VMEM((rows, width), F32),
            pltpu.VMEM((tiles, group, FT), BF16),
            pltpu.VMEM((2, tiles, group, FT), BF16),
            pltpu.VMEM((6, tiles, half, FT), BF16),
            pltpu.VMEM((2, tiles, half, FT), BF16),
            pltpu.VMEM((2, tiles, half, FT), BF16),
            pltpu.VMEM((tiles, half, FT), BF16),
            pltpu.VMEM((tiles, half, FT), BF16),
            dma((PSLOTS, w_proj.shape[0] // PT)), dma((hpad // HT,)), dma, dma((13, tiles + 1)), dma((13, tiles + 1)),
            dma((2, tiles)), dma((2, tiles)), dma((6, tiles)), dma((6, tiles)),
        ],
        compiler_params=pltpu.CompilerParams(vmem_limit_bytes=67043328, collective_id=0, has_side_effects=True),
        name='mlp_block',
    )(ctx, x_in, gamma_mlp, w_proj, w_in, w_out)


def solution(mesh):
    row_spec = P(('rep', 'grp'))
    repl_spec = P()

    def local_layer(x_in, seq_len, k_cache, v_cache, gamma_attn, w_qkv, b_qkv, w_proj, gamma_mlp, w_in, w_out):
        ctx, k_out, v_out = attention_block(x_in, seq_len, k_cache, v_cache, gamma_attn, w_qkv, b_qkv)
        layer_out = mlp_block(ctx, x_in, gamma_mlp, w_proj, w_in, w_out)
        return layer_out, k_out, v_out

    return jax.shard_map(local_layer, mesh=mesh,
                         in_specs=(row_spec, row_spec, row_spec, row_spec, repl_spec, repl_spec, repl_spec,
                                   repl_spec, repl_spec, P(None, 'grp', None), P('grp', None)),
                         out_specs=(row_spec, row_spec, row_spec), check_vma=False)
```

```python
import math

import jax
import jax.numpy as jnp
from jax import lax
from jax.experimental import pallas as pl
from jax.experimental.pallas import tpu as pltpu
from jax.sharding import PartitionSpec as P

HEAD_DIM = 128
ROT_DIM = HEAD_DIM // 2
ROPE_BASE = 10000.0
EPS = 1e-5
F32 = jnp.float32
BF16 = jnp.bfloat16

TN = 512
NW = 4
SG = 4
NS = 8
LAG = 3


def norm(vals, gain):
    mean_sq = jnp.mean(vals * vals, axis=-1, keepdims=True)
    return (vals * lax.rsqrt(mean_sq + EPS) * gain.astype(F32)).astype(BF16)


def attention_kernel(len_ref, x_ref, ga_ref, b_ref, kc, vc, wq,
                     ctx_ref, ko, vo,
                     wbuf, kbuf, vbuf, nbuf, bias, cos, sin, qh, qs, kn, vn, cb, colpos, wsem, insem, outsem):
    rows = x_ref.shape[0]
    heads = qh.shape[0]
    q_tiles = heads * HEAD_DIM // TN
    groups = rows // SG
    per_tile = TN // HEAD_DIM
    span = kbuf.shape[2]

    def q_copy(tile):
        slot = lax.rem(tile, NW)
        cols = pl.ds(pl.multiple_of(tile * TN, TN), TN)
        return pltpu.make_async_copy(wq.at[:, cols], wbuf.at[slot], wsem.at[slot])

    def cache_in(group):
        slot = lax.rem(group, NS)
        seqs = pl.ds(group * SG, SG)
        return (pltpu.make_async_copy(kc.at[seqs], kbuf.at[slot], insem.at[slot, 0]),
                pltpu.make_async_copy(vc.at[seqs], vbuf.at[slot], insem.at[slot, 1]))

    def cache_out(group):
        slot = lax.rem(group, NS)
        seqs = pl.ds(group * SG, SG)
        return (pltpu.make_async_copy(kbuf.at[slot], ko.at[seqs], outsem.at[slot, 0]),
                pltpu.make_async_copy(vbuf.at[slot], vo.at[seqs], outsem.at[slot, 1]))

    for t in range(NW):
        q_copy(t).start()

    row_id = lax.broadcasted_iota(jnp.int32, (heads, span), 0)
    col_id = lax.broadcasted_iota(jnp.int32, (heads, span), 1)
    kv_of_row = row_id // (heads // 2)
    colpos[...] = jnp.where((col_id & 1) == kv_of_row, col_id >> 1, span)

    nbuf[...] = norm(x_ref[...].astype(F32), ga_ref[...].astype(F32)[None, :])
    bias[...] = b_ref[...].astype(F32)[None, :]
    dim = lax.broadcasted_iota(jnp.int32, (1, HEAD_DIM), 1)
    freq = jnp.exp((dim - (dim & 1)).astype(F32) * (-math.log(ROPE_BASE) / ROT_DIM))
    freq = jnp.where(dim < ROT_DIM, freq, 0.0)
    for i in range(rows):
        cos[i:i + 1, :] = len_ref[i].astype(F32) * freq
    angles = cos[...]
    sign = jnp.where((dim & 1) == 0, -1.0, 1.0)
    cos[...] = jnp.cos(angles)
    sin[...] = jnp.sin(angles) * sign

    lane = lax.broadcasted_iota(jnp.int32, (rows, HEAD_DIM), 1)
    even = (lane & 1) == 0

    def rope(v):
        swapped = jnp.where(even, pltpu.roll(v, HEAD_DIM - 1, 1), pltpu.roll(v, 1, 1))
        return v * cos[...] + swapped * sin[...]

    def qkv_tile(tile):
        q_copy(tile).wait()
        cols = pl.ds(pl.multiple_of(tile * TN, TN), TN)
        out = jnp.dot(nbuf[...], wbuf[lax.rem(tile, NW)], preferred_element_type=F32)
        return out + bias[:, cols]

    def q_step(tile, carry):
        out = qkv_tile(tile)
        for i in range(per_tile):
            qh[tile * per_tile + i] = rope(out[:, i * HEAD_DIM:(i + 1) * HEAD_DIM])

        @pl.when(tile + NW < q_tiles + 1)
        def _():
            q_copy(tile + NW).start()

        @pl.when(tile + NW >= q_tiles + 1)
        def _():
            first = (tile + NW - q_tiles - 1) * 2
            for g in range(2):
                for c in cache_in(first + g):
                    c.start()
        return carry

    lax.fori_loop(0, q_tiles, q_step, 0)
    out = qkv_tile(q_tiles)
    for g in range(2):
        for c in cache_in((NW - 1) * 2 + g):
            c.start()
    for g in range(2):
        kn[g] = rope(out[:, g * HEAD_DIM:(g + 1) * HEAD_DIM])
        vn[g] = out[:, (2 + g) * HEAD_DIM:(3 + g) * HEAD_DIM]
    for hd in range(heads):
        qs[:, hd, :] = qh[hd]

    sub = lax.broadcasted_iota(jnp.int32, (16, HEAD_DIM), 0)
    scale = HEAD_DIM ** -0.5

    def group_step(group, carry):
        slot = lax.rem(group, NS)
        for c in cache_in(group):
            c.wait()
        for j in range(SG):
            seq = group * SG + j
            length = len_ref[seq]
            start = pl.multiple_of((length // 8) * 16, 16)
            here = (sub >> 1) == (length - (length // 8) * 8)
            for buf, new in ((kbuf, kn), (vbuf, vn)):
                pattern = jnp.where((sub & 1) == 0, new[0, pl.ds(seq, 1), :], new[1, pl.ds(seq, 1), :])
                old = buf[slot, j, pl.ds(start, 16), :].astype(F32)
                buf[slot, j, pl.ds(start, 16), :] = jnp.where(here, pattern, old).astype(BF16)
        for c in cache_out(group):
            c.start()
        dims = (((1,), (1,)), ((), ()))
        seqs = [group * SG + j for j in range(SG)]
        scores = [lax.dot_general(qs[seqs[j]].astype(BF16), kbuf[slot, j], dims, preferred_element_type=F32) * scale
                  for j in range(SG)]
        scores = [jnp.where(colpos[...] <= len_ref[seqs[j]], scores[j], -jnp.inf) for j in range(SG)]
        tops = [jnp.max(v, axis=-1, keepdims=True) for v in scores]
        weights = [jnp.exp(v - t) for v, t in zip(scores, tops)]
        totals = [jnp.sum(v, axis=-1, keepdims=True) for v in weights]
        probs = [(v / t).astype(BF16) for v, t in zip(weights, totals)]
        for j in range(SG):
            cb[seqs[j]] = jnp.dot(probs[j], vbuf[slot, j], preferred_element_type=F32)

        @pl.when(group >= LAG)
        def _():
            for c in cache_out(group - LAG):
                c.wait()

        @pl.when(jnp.logical_and(group >= LAG, group - LAG + NS < groups))
        def _():
            for c in cache_in(group - LAG + NS):
                c.start()

        return carry

    lax.fori_loop(0, groups, group_step, 0)
    for hd in range(heads):
        ctx_ref[:, hd * HEAD_DIM:(hd + 1) * HEAD_DIM] = cb[:, hd, :].astype(BF16)
    for g in range(LAG):
        for c in cache_out(groups - LAG + g):
            c.wait()


def attention_block(x_in, seq_len, k_cache, v_cache, gamma_attn, w_qkv, b_qkv):
    rows, width = x_in.shape
    cache_len, kv_heads = k_cache.shape[1], k_cache.shape[2]
    q_width = w_qkv.shape[1] - 2 * kv_heads * HEAD_DIM
    heads = q_width // HEAD_DIM
    span = cache_len * kv_heads
    flat = (rows, span, HEAD_DIM)
    vmem = pl.BlockSpec(memory_space=pltpu.VMEM)
    hbm = pl.BlockSpec(memory_space=pl.ANY)
    ctx, k_out, v_out = pl.pallas_call(
        attention_kernel,
        out_shape=(jax.ShapeDtypeStruct((rows, q_width), BF16),
                   jax.ShapeDtypeStruct(flat, BF16), jax.ShapeDtypeStruct(flat, BF16)),
        in_specs=[pl.BlockSpec(memory_space=pltpu.SMEM)] + [vmem] * 3 + [hbm] * 3,
        out_specs=(vmem, hbm, hbm),
        scratch_shapes=[
            pltpu.VMEM((NW, width, TN), BF16),
            pltpu.VMEM((NS, SG, span, HEAD_DIM), BF16),
            pltpu.VMEM((NS, SG, span, HEAD_DIM), BF16),
            pltpu.VMEM((rows, width), BF16),
            pltpu.VMEM((1, w_qkv.shape[1]), F32),
            pltpu.VMEM((rows, HEAD_DIM), F32),
            pltpu.VMEM((rows, HEAD_DIM), F32),
            pltpu.VMEM((heads, rows, HEAD_DIM), F32),
            pltpu.VMEM((rows, heads, HEAD_DIM), F32),
            pltpu.VMEM((kv_heads, rows, HEAD_DIM), F32),
            pltpu.VMEM((kv_heads, rows, HEAD_DIM), F32),
            pltpu.VMEM((rows, heads, HEAD_DIM), F32),
            pltpu.VMEM((heads, span), jnp.int32),
            pltpu.SemaphoreType.DMA((NW,)),
            pltpu.SemaphoreType.DMA((NS, 2)),
            pltpu.SemaphoreType.DMA((NS, 2)),
        ],
        compiler_params=pltpu.CompilerParams(vmem_limit_bytes=56 * 1024 * 1024),
        name='attention_block',
    )(seq_len, x_in, gamma_attn, b_qkv, k_cache.reshape(flat), v_cache.reshape(flat), w_qkv)
    return ctx, k_out.reshape(k_cache.shape), v_out.reshape(v_cache.shape)


FT = 1024
HT = 256


PT = 512
PSLOTS = 6
AHEAD = 2
HOP = 4
FAR = 3
SHIFT = 2.0 ** 64


def mlp_kernel(ctx_in, x_in, gm_in, wp, wi, wo, out_ref,
               gs, rows_all, rs_all, wib, wob, gbuf, facc, acc, topart, frompart, outbox,
               from_l, from_r, mid_l, mid_r,
               psem, wsem, osem, gsend, grecv, psend, precv, bsend, brecv):
    me = lax.axis_index('grp')
    chips = lax.axis_size('grp') // 2
    chip, core = me // 2, me % 2
    right = lax.rem(chip + 1, chips) * 2 + core
    left = lax.rem(chip + chips - 1, chips) * 2 + core
    partner = chip * 2 + 1 - core
    r = x_in.shape[0]
    s, g, br = r // 2, 2 * r, 4 * r
    hidden = wo.shape[0]
    full = hidden // HT
    rest = hidden - full * HT
    hpad = wob.shape[0]
    tiles = wo.shape[1] // FT

    def w_copy(j):
        part = pl.ds(pl.multiple_of(j * HT, HT), HT)
        return pltpu.make_async_copy(wi.at[:, part], wib.at[:, part], wsem.at[j])

    last_in = pltpu.make_async_copy(wi.at[:, pl.ds(full * HT, rest)], wib.at[:, pl.ds(full * HT, rest)], wsem.at[full])
    o_copy = pltpu.make_async_copy(wo, wob.at[pl.ds(0, hidden)], osem)
    p_tiles = wp.shape[1] // PT
    depth = wp.shape[0] // PT

    def p_part(t, k):
        slot = t % PSLOTS
        buf, row = (wob, slot * PT) if slot < PSLOTS // 2 else (wib.at[1], (slot - PSLOTS // 2) * PT)
        return buf.at[pl.ds(row, PT), pl.ds(k * PT, PT)]

    def p_copy(t, k):
        return pltpu.make_async_copy(wp.at[pl.ds(k * PT, PT), pl.ds(t * PT, PT)], p_part(t, k), psem.at[t % PSLOTS, k])

    for t in range(AHEAD):
        for k in range(depth):
            p_copy(t, k).start()
    gs[...] = gm_in[...].astype(F32)[None, :] * (1.0 / SHIFT)

    barrier = pltpu.get_barrier_semaphore()
    for dev in (right, left, partner):
        pl.semaphore_signal(barrier, inc=1, device_id={'grp': dev}, device_id_type=pl.DeviceIdType.MESH)
    pl.semaphore_wait(barrier, 3)

    def remote(src, dst, send, recv, dev):
        return pltpu.make_async_remote_copy(src_ref=src, dst_ref=dst, send_sem=send, recv_sem=recv,
                                            device_id={'grp': dev}, device_id_type=pl.DeviceIdType.MESH)

    def gather(n, src, dst, count, dev):
        def at(c):
            def view(first):
                if c == p_tiles:
                    return rs_all.at[pl.ds(first, count)]
                return rows_all.at[pl.ds(first, count), pl.ds(c * PT, PT)]
            return remote(view(src), view(dst), gsend.at[n, c], grecv.at[n, c], dev)
        return at

    to_r0 = gather(0, br, r, s, right)
    to_l1 = gather(1, br + s, r + s, s, left)
    to_r1 = gather(2, br + s, br + r, s, right)
    to_l0 = gather(3, br, br + r + s, s, left)
    to_p = gather(4, br, br + g, r, partner)
    on_r = gather(5, r, 0, s, right)
    on_l = gather(6, r + s, s, s, left)
    p_l0 = gather(7, r, g + r, s, partner)
    p_r1 = gather(8, r + s, g + r + s, s, partner)
    p_l1 = gather(9, br + r, br + g + r, s, partner)
    p_r0 = gather(10, br + r + s, br + g + r + s, s, partner)
    p_o0 = gather(11, 0, g, s, partner)
    p_o1 = gather(12, s, g + s, s, partner)
    gathers = [to_r0, to_l1, to_r1, to_l0, to_p, on_r, on_l, p_l0, p_r1, p_l1, p_r0, p_o0, p_o1]

    def pass_first(c):
        to_r0(c).wait_recv()
        on_r(c).start()
        p_l0(c).start()
        to_l1(c).wait_recv()
        on_l(c).start()
        p_r1(c).start()

    def pass_second(c):
        to_r1(c).wait_recv()
        p_l1(c).start()
        to_l0(c).wait_recv()
        p_r0(c).start()

    def pass_far(c):
        on_r(c).wait_recv()
        p_o0(c).start()
        on_l(c).wait_recv()
        p_o1(c).start()

    if hpad > hidden:
        wib[:, hidden:, :] = jnp.zeros((2, hpad - hidden, wib.shape[2]), BF16)
        wob[hidden:, :] = jnp.zeros((hpad - hidden, wob.shape[1]), BF16)

    square = jnp.zeros((r, HEAD_DIM), F32)
    for t in range(p_tiles):
        part = slice(t * PT, (t + 1) * PT)
        out = None
        for k in range(depth):
            p_copy(t, k).wait()
        if t + AHEAD < p_tiles:
            for k in range(depth):
                p_copy(t + AHEAD, k).start()
        for k in range(depth):
            term = jnp.dot(ctx_in[:, k * PT:(k + 1) * PT], p_part(t, k)[...], preferred_element_type=F32)
            out = term if out is None else out + term
        hid = x_in[:, part].astype(F32) + out
        acc[:, part] = hid
        rows_all[br:br + r, part] = (hid * gs[:, part]).astype(BF16)
        for copy in (to_r0, to_l1, to_p):
            copy(t).start()
        if t < HOP:
            to_r1(t).start()
            to_l0(t).start()
        for k in range(PT // HEAD_DIM):
            lanes = hid[:, k * HEAD_DIM:(k + 1) * HEAD_DIM]
            square = square + lanes * lanes
        if t == p_tiles - 2:
            w_copy(0).start()
        if t >= HOP:
            pass_first(t - HOP)
            pass_second(t - HOP)
        if t >= HOP + FAR:
            pass_far(t - HOP - FAR)
    for j in range(1, full):
        w_copy(j).start()
    if rest:
        last_in.start()
    o_copy.start()
    mean_sq = jnp.sum(square, axis=-1, keepdims=True) / wp.shape[1]
    rs_all[br:br + r, :] = jnp.broadcast_to(lax.rsqrt(mean_sq + EPS) * SHIFT, (r, HEAD_DIM))
    for copy in (to_r0, to_l1, to_p):
        copy(p_tiles).start()
    for c in range(p_tiles - HOP, p_tiles + 1):
        pass_first(c)
        to_r1(c).start()
        to_l0(c).start()
        pass_far(c - FAR)
    for c in range(p_tiles - FAR + 1, p_tiles + 1):
        pass_far(c)
    for c in range(p_tiles + 1):
        for copy in (p_l0, p_r1, p_o0, p_o1):
            copy(c).wait_recv()

    def gate_tile(blk, j):
        part = pl.ds(pl.multiple_of(j * HT, HT), HT)
        x = rows_all[pl.ds(blk * br, br)]
        dims = (((1,), (1,)), ((), ()))
        gate = lax.dot_general(x, wib[0, part, :], dims, preferred_element_type=F32)
        up = lax.dot_general(x, wib[1, part, :], dims, preferred_element_type=F32)
        scale = rs_all[pl.ds(blk * br, br), 0:1]
        gate = jnp.where(scale > 0.0, gate * scale, 0.0)
        up = jnp.where(scale > 0.0, up * scale, 0.0)
        gbuf[:, part] = (jax.nn.silu(gate) * up).astype(BF16)

    def cols(t):
        return slice(t * FT, (t + 1) * FT)

    def to_partner(blk, t):
        return remote(topart.at[t], frompart.at[blk, t], psend.at[blk, t], precv.at[blk, t], partner)

    def out_copy(kind, t):
        dst = (from_r.at[0, t], from_l.at[1, t], mid_l.at[t], mid_r.at[t], from_l.at[0, t], from_r.at[1, t])[kind]
        dev = (left, right, right, left, right, left)[kind]
        return remote(outbox.at[kind, t], dst, bsend.at[kind, t], brecv.at[kind, t], dev)

    def post(kind, t, vals):
        outbox[kind, t] = vals.astype(BF16)
        out_copy(kind, t).start()

    def down_tile(blk, t):
        f = jnp.dot(gbuf[...], wob[:, cols(t)], preferred_element_type=F32)
        if blk == 1:
            to_partner(0, t).wait_send()
        topart[t] = f[g:].astype(BF16)
        to_partner(blk, t).start()
        facc[t % 3] = f[:g]

    def finish(blk, t):
        to_partner(blk, t).wait_recv()
        total = facc[t % 3] + frompart[blk, t].astype(F32)
        if blk == 0:
            post(2, t, total[:s])
            post(3, t, total[s:r])
            post(0, t, total[r:r + s])
            post(1, t, total[r + s:])
        else:
            acc[:, cols(t)] += total[:r]
            out_copy(2, t).wait_recv()
            post(4, t, total[r + s:] + mid_l[t].astype(F32))
            out_copy(3, t).wait_recv()
            post(5, t, total[r:r + s] + mid_r[t].astype(F32))

    def first_step(j, carry):
        w_copy(j).wait()
        gate_tile(0, j)
        return carry

    def second_step(j, carry):
        gate_tile(1, j)
        return carry

    lax.fori_loop(0, full, first_step, 0)
    if rest:
        last_in.wait()
        gate_tile(0, full)
    for c in range(HOP, p_tiles + 1):
        pass_second(c)
    o_copy.wait()
    for t in range(tiles):
        down_tile(0, t)
        if t >= 2:
            finish(0, t - 2)
    finish(0, tiles - 2)
    for c in range(p_tiles + 1):
        for copy in (to_p, p_l1, p_r0):
            copy(c).wait_recv()
    gate_tile(1, 0)
    finish(0, tiles - 1)
    lax.fori_loop(1, hpad // HT, second_step, 0)
    for t in range(tiles):
        down_tile(1, t)
        if t:
            finish(1, t - 1)
    finish(1, tiles - 1)
    for t in range(tiles):
        for kind in (0, 1, 4, 5):
            out_copy(kind, t).wait_recv()
        for half in range(2):
            part = slice(half * s, (half + 1) * s)
            total = acc[part, cols(t)] + (from_l[half, t].astype(F32) + from_r[half, t].astype(F32))
            out_ref[part, cols(t)] = total.astype(BF16)
    for copy in gathers:
        for c in range(p_tiles + 1):
            copy(c).wait_send()
    for t in range(tiles):
        to_partner(1, t).wait_send()
        for kind in range(6):
            out_copy(kind, t).wait_send()


def mlp_block(ctx, x_in, gamma_mlp, w_proj, w_in, w_out):
    rows, width = x_in.shape
    hidden = w_out.shape[0]
    hpad = -(-hidden // HT) * HT
    tiles = width // FT
    half, group, block = rows // 2, 2 * rows, 4 * rows
    hbm = pl.BlockSpec(memory_space=pl.ANY)
    vmem = pl.BlockSpec(memory_space=pltpu.VMEM)
    dma = pltpu.SemaphoreType.DMA
    return pl.pallas_call(
        mlp_kernel,
        out_shape=jax.ShapeDtypeStruct((rows, width), BF16),
        in_specs=[vmem] * 3 + [hbm] * 3,
        out_specs=vmem,
        scratch_shapes=[
            pltpu.VMEM((1, width), F32),
            pltpu.VMEM((2 * block, width), BF16),
            pltpu.VMEM((2 * block, HEAD_DIM), F32),
            pltpu.VMEM((2, hpad, width), BF16),
            pltpu.VMEM((hpad, width), BF16),
            pltpu.VMEM((block, hpad), BF16),
            pltpu.VMEM((3, group, FT), F32),
            pltpu.VMEM((rows, width), F32),
            pltpu.VMEM((tiles, group, FT), BF16),
            pltpu.VMEM((2, tiles, group, FT), BF16),
            pltpu.VMEM((6, tiles, half, FT), BF16),
            pltpu.VMEM((2, tiles, half, FT), BF16),
            pltpu.VMEM((2, tiles, half, FT), BF16),
            pltpu.VMEM((tiles, half, FT), BF16),
            pltpu.VMEM((tiles, half, FT), BF16),
            dma((PSLOTS, w_proj.shape[0] // PT)), dma((hpad // HT,)), dma, dma((13, width // PT + 1)), dma((13, width // PT + 1)),
            dma((2, tiles)), dma((2, tiles)), dma((6, tiles)), dma((6, tiles)),
        ],
        compiler_params=pltpu.CompilerParams(vmem_limit_bytes=67043328, collective_id=0, has_side_effects=True),
        name='mlp_block',
    )(ctx, x_in, gamma_mlp, w_proj, w_in, w_out)


def solution(mesh):
    row_spec = P(('rep', 'grp'))
    repl_spec = P()

    def local_layer(x_in, seq_len, k_cache, v_cache, gamma_attn, w_qkv, b_qkv, w_proj, gamma_mlp, w_in, w_out):
        ctx, k_out, v_out = attention_block(x_in, seq_len, k_cache, v_cache, gamma_attn, w_qkv, b_qkv)
        layer_out = mlp_block(ctx, x_in, gamma_mlp, w_proj, w_in, w_out)
        return layer_out, k_out, v_out

    return jax.shard_map(local_layer, mesh=mesh,
                         in_specs=(row_spec, row_spec, row_spec, row_spec, repl_spec, repl_spec, repl_spec,
                                   repl_spec, repl_spec, P(None, 'grp', None), P('grp', None)),
                         out_specs=(row_spec, row_spec, row_spec), check_vma=False)
```

```python
import math

import jax
import jax.numpy as jnp
from jax import lax
from jax.experimental import pallas as pl
from jax.experimental.pallas import tpu as pltpu
from jax.sharding import PartitionSpec as P

HEAD_DIM = 128
ROT_DIM = HEAD_DIM // 2
ROPE_BASE = 10000.0
EPS = 1e-5
F32 = jnp.float32
BF16 = jnp.bfloat16

TN = 512
NW = 4
SG = 4
NS = 8
LAG = 3


def norm(vals, gain):
    mean_sq = jnp.mean(vals * vals, axis=-1, keepdims=True)
    return (vals * lax.rsqrt(mean_sq + EPS) * gain.astype(F32)).astype(BF16)


def attention_kernel(len_ref, x_ref, ga_ref, b_ref, kc, vc, wq,
                     ctx_ref, ko, vo,
                     wbuf, kbuf, vbuf, nbuf, bias, cos, sin, qh, qs, kn, vn, cb, colpos, wsem, insem, outsem):
    rows = x_ref.shape[0]
    heads = qh.shape[0]
    q_tiles = heads * HEAD_DIM // TN
    groups = rows // SG
    per_tile = TN // HEAD_DIM
    span = kbuf.shape[2]

    def q_copy(tile):
        slot = lax.rem(tile, NW)
        cols = pl.ds(pl.multiple_of(tile * TN, TN), TN)
        return pltpu.make_async_copy(wq.at[:, cols], wbuf.at[slot], wsem.at[slot])

    def cache_in(group):
        slot = lax.rem(group, NS)
        seqs = pl.ds(group * SG, SG)
        return (pltpu.make_async_copy(kc.at[seqs], kbuf.at[slot], insem.at[slot, 0]),
                pltpu.make_async_copy(vc.at[seqs], vbuf.at[slot], insem.at[slot, 1]))

    def cache_out(group):
        slot = lax.rem(group, NS)
        seqs = pl.ds(group * SG, SG)
        return (pltpu.make_async_copy(kbuf.at[slot], ko.at[seqs], outsem.at[slot, 0]),
                pltpu.make_async_copy(vbuf.at[slot], vo.at[seqs], outsem.at[slot, 1]))

    for t in range(NW):
        q_copy(t).start()

    row_id = lax.broadcasted_iota(jnp.int32, (heads, span), 0)
    col_id = lax.broadcasted_iota(jnp.int32, (heads, span), 1)
    kv_of_row = row_id // (heads // 2)
    colpos[...] = jnp.where((col_id & 1) == kv_of_row, col_id >> 1, span)

    nbuf[...] = norm(x_ref[...].astype(F32), ga_ref[...].astype(F32)[None, :])
    bias[...] = b_ref[...].astype(F32)[None, :]
    dim = lax.broadcasted_iota(jnp.int32, (1, HEAD_DIM), 1)
    freq = jnp.exp((dim - (dim & 1)).astype(F32) * (-math.log(ROPE_BASE) / ROT_DIM))
    freq = jnp.where(dim < ROT_DIM, freq, 0.0)
    for i in range(rows):
        cos[i:i + 1, :] = len_ref[i].astype(F32) * freq
    angles = cos[...]
    sign = jnp.where((dim & 1) == 0, -1.0, 1.0)
    cos[...] = jnp.cos(angles)
    sin[...] = jnp.sin(angles) * sign

    lane = lax.broadcasted_iota(jnp.int32, (rows, HEAD_DIM), 1)
    even = (lane & 1) == 0

    def rope(v):
        swapped = jnp.where(even, pltpu.roll(v, HEAD_DIM - 1, 1), pltpu.roll(v, 1, 1))
        return v * cos[...] + swapped * sin[...]

    def qkv_tile(tile):
        q_copy(tile).wait()
        cols = pl.ds(pl.multiple_of(tile * TN, TN), TN)
        out = jnp.dot(nbuf[...], wbuf[lax.rem(tile, NW)], preferred_element_type=F32)
        return out + bias[:, cols]

    def q_step(tile, carry):
        out = qkv_tile(tile)
        for i in range(per_tile):
            qh[tile * per_tile + i] = rope(out[:, i * HEAD_DIM:(i + 1) * HEAD_DIM])

        @pl.when(tile + NW < q_tiles + 1)
        def _():
            q_copy(tile + NW).start()

        @pl.when(tile + NW >= q_tiles + 1)
        def _():
            first = (tile + NW - q_tiles - 1) * 2
            for g in range(2):
                for c in cache_in(first + g):
                    c.start()
        return carry

    lax.fori_loop(0, q_tiles, q_step, 0)
    out = qkv_tile(q_tiles)
    for g in range(2):
        for c in cache_in((NW - 1) * 2 + g):
            c.start()
    for g in range(2):
        kn[g] = rope(out[:, g * HEAD_DIM:(g + 1) * HEAD_DIM])
        vn[g] = out[:, (2 + g) * HEAD_DIM:(3 + g) * HEAD_DIM]
    for hd in range(heads):
        qs[:, hd, :] = qh[hd]

    sub = lax.broadcasted_iota(jnp.int32, (16, HEAD_DIM), 0)
    scale = HEAD_DIM ** -0.5

    def group_step(group, carry):
        slot = lax.rem(group, NS)
        for c in cache_in(group):
            c.wait()
        for j in range(SG):
            seq = group * SG + j
            length = len_ref[seq]
            start = pl.multiple_of((length // 8) * 16, 16)
            here = (sub >> 1) == (length - (length // 8) * 8)
            for buf, new in ((kbuf, kn), (vbuf, vn)):
                pattern = jnp.where((sub & 1) == 0, new[0, pl.ds(seq, 1), :], new[1, pl.ds(seq, 1), :])
                old = buf[slot, j, pl.ds(start, 16), :].astype(F32)
                buf[slot, j, pl.ds(start, 16), :] = jnp.where(here, pattern, old).astype(BF16)
        for c in cache_out(group):
            c.start()
        dims = (((1,), (1,)), ((), ()))
        seqs = [group * SG + j for j in range(SG)]
        scores = [lax.dot_general(qs[seqs[j]].astype(BF16), kbuf[slot, j], dims, preferred_element_type=F32) * scale
                  for j in range(SG)]
        scores = [jnp.where(colpos[...] <= len_ref[seqs[j]], scores[j], -jnp.inf) for j in range(SG)]
        tops = [jnp.max(v, axis=-1, keepdims=True) for v in scores]
        weights = [jnp.exp(v - t) for v, t in zip(scores, tops)]
        totals = [jnp.sum(v, axis=-1, keepdims=True) for v in weights]
        probs = [(v / t).astype(BF16) for v, t in zip(weights, totals)]
        for j in range(SG):
            cb[seqs[j]] = jnp.dot(probs[j], vbuf[slot, j], preferred_element_type=F32)

        @pl.when(group >= LAG)
        def _():
            for c in cache_out(group - LAG):
                c.wait()

        @pl.when(jnp.logical_and(group >= LAG, group - LAG + NS < groups))
        def _():
            for c in cache_in(group - LAG + NS):
                c.start()

        return carry

    lax.fori_loop(0, groups, group_step, 0)
    for hd in range(heads):
        ctx_ref[:, hd * HEAD_DIM:(hd + 1) * HEAD_DIM] = cb[:, hd, :].astype(BF16)
    for g in range(LAG):
        for c in cache_out(groups - LAG + g):
            c.wait()


def attention_block(x_in, seq_len, k_cache, v_cache, gamma_attn, w_qkv, b_qkv):
    rows, width = x_in.shape
    cache_len, kv_heads = k_cache.shape[1], k_cache.shape[2]
    q_width = w_qkv.shape[1] - 2 * kv_heads * HEAD_DIM
    heads = q_width // HEAD_DIM
    span = cache_len * kv_heads
    flat = (rows, span, HEAD_DIM)
    vmem = pl.BlockSpec(memory_space=pltpu.VMEM)
    hbm = pl.BlockSpec(memory_space=pl.ANY)
    ctx, k_out, v_out = pl.pallas_call(
        attention_kernel,
        out_shape=(jax.ShapeDtypeStruct((rows, q_width), BF16),
                   jax.ShapeDtypeStruct(flat, BF16), jax.ShapeDtypeStruct(flat, BF16)),
        in_specs=[pl.BlockSpec(memory_space=pltpu.SMEM)] + [vmem] * 3 + [hbm] * 3,
        out_specs=(vmem, hbm, hbm),
        scratch_shapes=[
            pltpu.VMEM((NW, width, TN), BF16),
            pltpu.VMEM((NS, SG, span, HEAD_DIM), BF16),
            pltpu.VMEM((NS, SG, span, HEAD_DIM), BF16),
            pltpu.VMEM((rows, width), BF16),
            pltpu.VMEM((1, w_qkv.shape[1]), F32),
            pltpu.VMEM((rows, HEAD_DIM), F32),
            pltpu.VMEM((rows, HEAD_DIM), F32),
            pltpu.VMEM((heads, rows, HEAD_DIM), F32),
            pltpu.VMEM((rows, heads, HEAD_DIM), F32),
            pltpu.VMEM((kv_heads, rows, HEAD_DIM), F32),
            pltpu.VMEM((kv_heads, rows, HEAD_DIM), F32),
            pltpu.VMEM((rows, heads, HEAD_DIM), F32),
            pltpu.VMEM((heads, span), jnp.int32),
            pltpu.SemaphoreType.DMA((NW,)),
            pltpu.SemaphoreType.DMA((NS, 2)),
            pltpu.SemaphoreType.DMA((NS, 2)),
        ],
        compiler_params=pltpu.CompilerParams(vmem_limit_bytes=56 * 1024 * 1024),
        name='attention_block',
    )(seq_len, x_in, gamma_attn, b_qkv, k_cache.reshape(flat), v_cache.reshape(flat), w_qkv)
    return ctx, k_out.reshape(k_cache.shape), v_out.reshape(v_cache.shape)


FT = 1024
HT = 256


PT = 512
PSLOTS = 6
AHEAD = 2
HOP = 3
FAR = 3
SHIFT = 2.0 ** 64


def mlp_kernel(ctx_in, x_in, gm_in, wp, wi, wo, out_ref,
               gs, rows_all, rs_all, wib, wob, gbuf, facc, acc, topart, frompart, outbox,
               from_l, from_r, mid_l, mid_r,
               psem, wsem, osem, gsend, grecv, psend, precv, bsend, brecv):
    me = lax.axis_index('grp')
    chips = lax.axis_size('grp') // 2
    chip, core = me // 2, me % 2
    right = lax.rem(chip + 1, chips) * 2 + core
    left = lax.rem(chip + chips - 1, chips) * 2 + core
    partner = chip * 2 + 1 - core
    r = x_in.shape[0]
    s, g, br = r // 2, 2 * r, 4 * r
    hidden = wo.shape[0]
    full = hidden // HT
    rest = hidden - full * HT
    hpad = wob.shape[0]
    tiles = wo.shape[1] // FT

    def w_copy(j):
        part = pl.ds(pl.multiple_of(j * HT, HT), HT)
        return pltpu.make_async_copy(wi.at[:, part], wib.at[:, part], wsem.at[j])

    last_in = pltpu.make_async_copy(wi.at[:, pl.ds(full * HT, rest)], wib.at[:, pl.ds(full * HT, rest)], wsem.at[full])
    o_copy = pltpu.make_async_copy(wo, wob.at[pl.ds(0, hidden)], osem)
    p_tiles = wp.shape[1] // PT
    depth = wp.shape[0] // PT

    def p_part(t, k):
        slot = t % PSLOTS
        buf, row = (wob, slot * PT) if slot < PSLOTS // 2 else (wib.at[1], (slot - PSLOTS // 2) * PT)
        return buf.at[pl.ds(row, PT), pl.ds(k * PT, PT)]

    def p_copy(t, k):
        return pltpu.make_async_copy(wp.at[pl.ds(k * PT, PT), pl.ds(t * PT, PT)], p_part(t, k), psem.at[t % PSLOTS, k])

    for t in range(AHEAD):
        for k in range(depth):
            p_copy(t, k).start()
    gs[...] = gm_in[...].astype(F32)[None, :] * (1.0 / SHIFT)

    barrier = pltpu.get_barrier_semaphore()
    for dev in (right, left, partner):
        pl.semaphore_signal(barrier, inc=1, device_id={'grp': dev}, device_id_type=pl.DeviceIdType.MESH)
    pl.semaphore_wait(barrier, 3)

    def remote(src, dst, send, recv, dev):
        return pltpu.make_async_remote_copy(src_ref=src, dst_ref=dst, send_sem=send, recv_sem=recv,
                                            device_id={'grp': dev}, device_id_type=pl.DeviceIdType.MESH)

    def gather(n, src, dst, count, dev):
        def at(c):
            def view(first):
                if c == p_tiles:
                    return rs_all.at[pl.ds(first, count)]
                return rows_all.at[pl.ds(first, count), pl.ds(c * PT, PT)]
            return remote(view(src), view(dst), gsend.at[n, c], grecv.at[n, c], dev)
        return at

    to_r0 = gather(0, br, r, s, right)
    to_l1 = gather(1, br + s, r + s, s, left)
    to_r1 = gather(2, br + s, br + r, s, right)
    to_l0 = gather(3, br, br + r + s, s, left)
    to_p = gather(4, br, br + g, r, partner)
    on_r = gather(5, r, 0, s, right)
    on_l = gather(6, r + s, s, s, left)
    p_l0 = gather(7, r, g + r, s, partner)
    p_r1 = gather(8, r + s, g + r + s, s, partner)
    p_l1 = gather(9, br + r, br + g + r, s, partner)
    p_r0 = gather(10, br + r + s, br + g + r + s, s, partner)
    p_o0 = gather(11, 0, g, s, partner)
    p_o1 = gather(12, s, g + s, s, partner)
    gathers = [to_r0, to_l1, to_r1, to_l0, to_p, on_r, on_l, p_l0, p_r1, p_l1, p_r0, p_o0, p_o1]

    def pass_first(c):
        to_r0(c).wait_recv()
        on_r(c).start()
        p_l0(c).start()
        to_l1(c).wait_recv()
        on_l(c).start()
        p_r1(c).start()

    def pass_second(c):
        to_r1(c).wait_recv()
        p_l1(c).start()
        to_l0(c).wait_recv()
        p_r0(c).start()

    def pass_far(c):
        on_r(c).wait_recv()
        p_o0(c).start()
        on_l(c).wait_recv()
        p_o1(c).start()

    if hpad > hidden:
        wib[:, hidden:, :] = jnp.zeros((2, hpad - hidden, wib.shape[2]), BF16)
        wob[hidden:, :] = jnp.zeros((hpad - hidden, wob.shape[1]), BF16)

    square = jnp.zeros((r, HEAD_DIM), F32)
    for t in range(p_tiles):
        part = slice(t * PT, (t + 1) * PT)
        out = None
        for k in range(depth):
            p_copy(t, k).wait()
        if t + AHEAD < p_tiles:
            for k in range(depth):
                p_copy(t + AHEAD, k).start()
        for k in range(depth):
            term = jnp.dot(ctx_in[:, k * PT:(k + 1) * PT], p_part(t, k)[...], preferred_element_type=F32)
            out = term if out is None else out + term
        hid = x_in[:, part].astype(F32) + out
        acc[:, part] = hid
        rows_all[br:br + r, part] = (hid * gs[:, part]).astype(BF16)
        for copy in (to_r0, to_l1, to_p):
            copy(t).start()
        if t < HOP:
            to_r1(t).start()
            to_l0(t).start()
        for k in range(PT // HEAD_DIM):
            lanes = hid[:, k * HEAD_DIM:(k + 1) * HEAD_DIM]
            square = square + lanes * lanes
        if t == p_tiles - 2:
            w_copy(0).start()
        if t >= HOP:
            pass_first(t - HOP)
            if t - HOP < HOP:
                pass_second(t - HOP)
        if t >= HOP + FAR:
            pass_far(t - HOP - FAR)
    loads = [w_copy(j) for j in range(1, full)] + ([last_in] if rest else []) + [o_copy]
    mean_sq = jnp.sum(square, axis=-1, keepdims=True) / wp.shape[1]
    rs_all[br:br + r, :] = jnp.broadcast_to(lax.rsqrt(mean_sq + EPS) * SHIFT, (r, HEAD_DIM))
    for copy in (to_r0, to_l1, to_p):
        copy(p_tiles).start()
    for c in range(p_tiles - HOP, p_tiles + 1):
        for copy in loads[:2]:
            copy.start()
        loads = loads[2:]
        pass_first(c)
        pass_far(c - FAR)
    for copy in loads:
        copy.start()
    for c in range(HOP, p_tiles + 1):
        to_r1(c).start()
        to_l0(c).start()
    for c in range(p_tiles - FAR + 1, p_tiles + 1):
        pass_far(c)
    for c in range(p_tiles + 1):
        for copy in (p_l0, p_r1, p_o0, p_o1):
            copy(c).wait_recv()

    def gate_tile(blk, j):
        part = pl.ds(pl.multiple_of(j * HT, HT), HT)
        x = rows_all[pl.ds(blk * br, br)]
        dims = (((1,), (1,)), ((), ()))
        gate = lax.dot_general(x, wib[0, part, :], dims, preferred_element_type=F32)
        up = lax.dot_general(x, wib[1, part, :], dims, preferred_element_type=F32)
        scale = rs_all[pl.ds(blk * br, br), 0:1]
        gate = jnp.where(scale > 0.0, gate * scale, 0.0)
        up = jnp.where(scale > 0.0, up * scale, 0.0)
        gbuf[:, part] = (jax.nn.silu(gate) * up).astype(BF16)

    def cols(t):
        return slice(t * FT, (t + 1) * FT)

    def to_partner(blk, t):
        return remote(topart.at[t], frompart.at[blk, t], psend.at[blk, t], precv.at[blk, t], partner)

    def out_copy(kind, t):
        dst = (from_r.at[0, t], from_l.at[1, t], mid_l.at[t], mid_r.at[t], from_l.at[0, t], from_r.at[1, t])[kind]
        dev = (left, right, right, left, right, left)[kind]
        return remote(outbox.at[kind, t], dst, bsend.at[kind, t], brecv.at[kind, t], dev)

    def post(kind, t, vals):
        outbox[kind, t] = vals.astype(BF16)
        out_copy(kind, t).start()

    def down_tile(blk, t):
        f = jnp.dot(gbuf[...], wob[:, cols(t)], preferred_element_type=F32)
        if blk == 1:
            to_partner(0, t).wait_send()
        topart[t] = f[g:].astype(BF16)
        to_partner(blk, t).start()
        facc[t % 3] = f[:g]

    def finish(blk, t):
        to_partner(blk, t).wait_recv()
        total = facc[t % 3] + frompart[blk, t].astype(F32)
        if blk == 0:
            post(2, t, total[:s])
            post(3, t, total[s:r])
            post(0, t, total[r:r + s])
            post(1, t, total[r + s:])
        else:
            acc[:, cols(t)] += total[:r]
            out_copy(2, t).wait_recv()
            post(4, t, total[r + s:] + mid_l[t].astype(F32))
            out_copy(3, t).wait_recv()
            post(5, t, total[r:r + s] + mid_r[t].astype(F32))

    def first_step(j, carry):
        w_copy(j).wait()
        gate_tile(0, j)
        return carry

    def second_step(j, carry):
        gate_tile(1, j)
        return carry

    lax.fori_loop(0, full, first_step, 0)
    if rest:
        last_in.wait()
        gate_tile(0, full)
    for c in range(min(HOP, p_tiles - HOP), p_tiles + 1):
        pass_second(c)
    o_copy.wait()
    for t in range(tiles):
        down_tile(0, t)
        if t >= 2:
            finish(0, t - 2)
    finish(0, tiles - 2)
    for c in range(p_tiles + 1):
        for copy in (to_p, p_l1, p_r0):
            copy(c).wait_recv()
    gate_tile(1, 0)
    finish(0, tiles - 1)
    lax.fori_loop(1, hpad // HT, second_step, 0)
    for t in range(tiles):
        down_tile(1, t)
        if t:
            finish(1, t - 1)
    finish(1, tiles - 1)
    for t in range(tiles):
        for kind in (0, 1, 4, 5):
            out_copy(kind, t).wait_recv()
        for half in range(2):
            part = slice(half * s, (half + 1) * s)
            total = acc[part, cols(t)] + (from_l[half, t].astype(F32) + from_r[half, t].astype(F32))
            out_ref[part, cols(t)] = total.astype(BF16)
    for copy in gathers:
        for c in range(p_tiles + 1):
            copy(c).wait_send()
    for t in range(tiles):
        to_partner(1, t).wait_send()
        for kind in range(6):
            out_copy(kind, t).wait_send()


def mlp_block(ctx, x_in, gamma_mlp, w_proj, w_in, w_out):
    rows, width = x_in.shape
    hidden = w_out.shape[0]
    hpad = -(-hidden // HT) * HT
    tiles = width // FT
    half, group, block = rows // 2, 2 * rows, 4 * rows
    hbm = pl.BlockSpec(memory_space=pl.ANY)
    vmem = pl.BlockSpec(memory_space=pltpu.VMEM)
    dma = pltpu.SemaphoreType.DMA
    return pl.pallas_call(
        mlp_kernel,
        out_shape=pltpu.VMEM((rows, width), BF16),
        in_specs=[vmem] * 3 + [hbm] * 3,
        out_specs=vmem,
        scratch_shapes=[
            pltpu.VMEM((1, width), F32),
            pltpu.VMEM((2 * block, width), BF16),
            pltpu.VMEM((2 * block, HEAD_DIM), F32),
            pltpu.VMEM((2, hpad, width), BF16),
            pltpu.VMEM((hpad, width), BF16),
            pltpu.VMEM((block, hpad), BF16),
            pltpu.VMEM((3, group, FT), F32),
            pltpu.VMEM((rows, width), F32),
            pltpu.VMEM((tiles, group, FT), BF16),
            pltpu.VMEM((2, tiles, group, FT), BF16),
            pltpu.VMEM((6, tiles, half, FT), BF16),
            pltpu.VMEM((2, tiles, half, FT), BF16),
            pltpu.VMEM((2, tiles, half, FT), BF16),
            pltpu.VMEM((tiles, half, FT), BF16),
            pltpu.VMEM((tiles, half, FT), BF16),
            dma((PSLOTS, w_proj.shape[0] // PT)), dma((hpad // HT,)), dma, dma((13, width // PT + 1)), dma((13, width // PT + 1)),
            dma((2, tiles)), dma((2, tiles)), dma((6, tiles)), dma((6, tiles)),
        ],
        compiler_params=pltpu.CompilerParams(vmem_limit_bytes=60 * 1024 * 1024, collective_id=0, has_side_effects=True),
        name='mlp_block',
    )(ctx, x_in, gamma_mlp, w_proj, w_in, w_out)


def solution(mesh):
    row_spec = P(('rep', 'grp'))
    repl_spec = P()

    def local_layer(x_in, seq_len, k_cache, v_cache, gamma_attn, w_qkv, b_qkv, w_proj, gamma_mlp, w_in, w_out):
        ctx, k_out, v_out = attention_block(x_in, seq_len, k_cache, v_cache, gamma_attn, w_qkv, b_qkv)
        layer_out = mlp_block(ctx, x_in, gamma_mlp, w_proj, w_in, w_out)
        return layer_out, k_out, v_out

    return jax.shard_map(local_layer, mesh=mesh,
                         in_specs=(row_spec, row_spec, row_spec, row_spec, repl_spec, repl_spec, repl_spec,
                                   repl_spec, repl_spec, P(None, 'grp', None), P('grp', None)),
                         out_specs=(row_spec, row_spec, row_spec), check_vma=False)
```

```python
import math

import jax
import jax.numpy as jnp
from jax import lax
from jax.experimental import pallas as pl
from jax.experimental.pallas import tpu as pltpu
from jax.sharding import PartitionSpec as P

HEAD_DIM = 128
ROT_DIM = HEAD_DIM // 2
ROPE_BASE = 10000.0
EPS = 1e-5
F32 = jnp.float32
BF16 = jnp.bfloat16

TN = 512
NW = 4
SG = 4
NS = 8
LAG = 3


def norm(vals, gain):
    mean_sq = jnp.mean(vals * vals, axis=-1, keepdims=True)
    return (vals * lax.rsqrt(mean_sq + EPS) * gain.astype(F32)).astype(BF16)


def attention_kernel(len_ref, x_ref, ga_ref, b_ref, kc, vc, wq,
                     ctx_ref, ko, vo,
                     wbuf, kbuf, vbuf, nbuf, bias, cos, sin, qh, qs, kn, vn, cb, colpos, wsem, insem, outsem):
    rows = x_ref.shape[0]
    heads = qh.shape[0]
    q_tiles = heads * HEAD_DIM // TN
    groups = rows // SG
    per_tile = TN // HEAD_DIM
    span = kbuf.shape[2]

    def q_copy(tile):
        slot = lax.rem(tile, NW)
        cols = pl.ds(pl.multiple_of(tile * TN, TN), TN)
        return pltpu.make_async_copy(wq.at[:, cols], wbuf.at[slot], wsem.at[slot])

    def cache_in(group):
        slot = lax.rem(group, NS)
        seqs = pl.ds(group * SG, SG)
        return (pltpu.make_async_copy(kc.at[seqs], kbuf.at[slot], insem.at[slot, 0]),
                pltpu.make_async_copy(vc.at[seqs], vbuf.at[slot], insem.at[slot, 1]))

    def cache_out(group):
        slot = lax.rem(group, NS)
        seqs = pl.ds(group * SG, SG)
        return (pltpu.make_async_copy(kbuf.at[slot], ko.at[seqs], outsem.at[slot, 0]),
                pltpu.make_async_copy(vbuf.at[slot], vo.at[seqs], outsem.at[slot, 1]))

    for t in range(NW):
        q_copy(t).start()

    row_id = lax.broadcasted_iota(jnp.int32, (heads, span), 0)
    col_id = lax.broadcasted_iota(jnp.int32, (heads, span), 1)
    kv_of_row = row_id // (heads // 2)
    colpos[...] = jnp.where((col_id & 1) == kv_of_row, col_id >> 1, span)

    nbuf[...] = norm(x_ref[...].astype(F32), ga_ref[...].astype(F32)[None, :])
    bias[...] = b_ref[...].astype(F32)[None, :]
    dim = lax.broadcasted_iota(jnp.int32, (1, HEAD_DIM), 1)
    freq = jnp.exp((dim - (dim & 1)).astype(F32) * (-math.log(ROPE_BASE) / ROT_DIM))
    freq = jnp.where(dim < ROT_DIM, freq, 0.0)
    for i in range(rows):
        cos[i:i + 1, :] = len_ref[i].astype(F32) * freq
    angles = cos[...]
    sign = jnp.where((dim & 1) == 0, -1.0, 1.0)
    cos[...] = jnp.cos(angles)
    sin[...] = jnp.sin(angles) * sign

    lane = lax.broadcasted_iota(jnp.int32, (rows, HEAD_DIM), 1)
    even = (lane & 1) == 0

    def rope(v):
        swapped = jnp.where(even, pltpu.roll(v, HEAD_DIM - 1, 1), pltpu.roll(v, 1, 1))
        return v * cos[...] + swapped * sin[...]

    def qkv_tile(tile):
        q_copy(tile).wait()
        cols = pl.ds(pl.multiple_of(tile * TN, TN), TN)
        out = jnp.dot(nbuf[...], wbuf[lax.rem(tile, NW)], preferred_element_type=F32)
        return out + bias[:, cols]

    def q_step(tile, carry):
        out = qkv_tile(tile)
        for i in range(per_tile):
            qh[tile * per_tile + i] = rope(out[:, i * HEAD_DIM:(i + 1) * HEAD_DIM])

        @pl.when(tile + NW < q_tiles + 1)
        def _():
            q_copy(tile + NW).start()

        @pl.when(tile + NW >= q_tiles + 1)
        def _():
            first = (tile + NW - q_tiles - 1) * 2
            for g in range(2):
                for c in cache_in(first + g):
                    c.start()
        return carry

    lax.fori_loop(0, q_tiles, q_step, 0)
    out = qkv_tile(q_tiles)
    for g in range(2):
        for c in cache_in((NW - 1) * 2 + g):
            c.start()
    for g in range(2):
        kn[g] = rope(out[:, g * HEAD_DIM:(g + 1) * HEAD_DIM])
        vn[g] = out[:, (2 + g) * HEAD_DIM:(3 + g) * HEAD_DIM]
    for hd in range(heads):
        qs[:, hd, :] = qh[hd]

    sub = lax.broadcasted_iota(jnp.int32, (16, HEAD_DIM), 0)
    scale = HEAD_DIM ** -0.5

    def group_step(group, carry):
        slot = lax.rem(group, NS)
        for c in cache_in(group):
            c.wait()
        for j in range(SG):
            seq = group * SG + j
            length = len_ref[seq]
            start = pl.multiple_of((length // 8) * 16, 16)
            here = (sub >> 1) == (length - (length // 8) * 8)
            for buf, new in ((kbuf, kn), (vbuf, vn)):
                pattern = jnp.where((sub & 1) == 0, new[0, pl.ds(seq, 1), :], new[1, pl.ds(seq, 1), :])
                old = buf[slot, j, pl.ds(start, 16), :].astype(F32)
                buf[slot, j, pl.ds(start, 16), :] = jnp.where(here, pattern, old).astype(BF16)
        for c in cache_out(group):
            c.start()
        dims = (((1,), (1,)), ((), ()))
        seqs = [group * SG + j for j in range(SG)]
        scores = [lax.dot_general(qs[seqs[j]].astype(BF16), kbuf[slot, j], dims, preferred_element_type=F32) * scale
                  for j in range(SG)]
        scores = [jnp.where(colpos[...] <= len_ref[seqs[j]], scores[j], -jnp.inf) for j in range(SG)]
        tops = [jnp.max(v, axis=-1, keepdims=True) for v in scores]
        weights = [jnp.exp(v - t) for v, t in zip(scores, tops)]
        totals = [jnp.sum(v, axis=-1, keepdims=True) for v in weights]
        probs = [(v / t).astype(BF16) for v, t in zip(weights, totals)]
        for j in range(SG):
            cb[seqs[j]] = jnp.dot(probs[j], vbuf[slot, j], preferred_element_type=F32)

        @pl.when(group >= LAG)
        def _():
            for c in cache_out(group - LAG):
                c.wait()

        @pl.when(jnp.logical_and(group >= LAG, group - LAG + NS < groups))
        def _():
            for c in cache_in(group - LAG + NS):
                c.start()

        return carry

    lax.fori_loop(0, groups, group_step, 0)
    for hd in range(heads):
        ctx_ref[:, hd * HEAD_DIM:(hd + 1) * HEAD_DIM] = cb[:, hd, :].astype(BF16)
    for g in range(LAG):
        for c in cache_out(groups - LAG + g):
            c.wait()


def attention_block(x_in, seq_len, k_cache, v_cache, gamma_attn, w_qkv, b_qkv):
    rows, width = x_in.shape
    cache_len, kv_heads = k_cache.shape[1], k_cache.shape[2]
    q_width = w_qkv.shape[1] - 2 * kv_heads * HEAD_DIM
    heads = q_width // HEAD_DIM
    span = cache_len * kv_heads
    flat = (rows, span, HEAD_DIM)
    vmem = pl.BlockSpec(memory_space=pltpu.VMEM)
    hbm = pl.BlockSpec(memory_space=pl.ANY)
    ctx, k_out, v_out = pl.pallas_call(
        attention_kernel,
        out_shape=(pltpu.VMEM((rows, q_width), BF16),
                   jax.ShapeDtypeStruct(flat, BF16), jax.ShapeDtypeStruct(flat, BF16)),
        in_specs=[pl.BlockSpec(memory_space=pltpu.SMEM)] + [vmem] * 3 + [hbm] * 3,
        out_specs=(vmem, hbm, hbm),
        scratch_shapes=[
            pltpu.VMEM((NW, width, TN), BF16),
            pltpu.VMEM((NS, SG, span, HEAD_DIM), BF16),
            pltpu.VMEM((NS, SG, span, HEAD_DIM), BF16),
            pltpu.VMEM((rows, width), BF16),
            pltpu.VMEM((1, w_qkv.shape[1]), F32),
            pltpu.VMEM((rows, HEAD_DIM), F32),
            pltpu.VMEM((rows, HEAD_DIM), F32),
            pltpu.VMEM((heads, rows, HEAD_DIM), F32),
            pltpu.VMEM((rows, heads, HEAD_DIM), F32),
            pltpu.VMEM((kv_heads, rows, HEAD_DIM), F32),
            pltpu.VMEM((kv_heads, rows, HEAD_DIM), F32),
            pltpu.VMEM((rows, heads, HEAD_DIM), F32),
            pltpu.VMEM((heads, span), jnp.int32),
            pltpu.SemaphoreType.DMA((NW,)),
            pltpu.SemaphoreType.DMA((NS, 2)),
            pltpu.SemaphoreType.DMA((NS, 2)),
        ],
        compiler_params=pltpu.CompilerParams(vmem_limit_bytes=56 * 1024 * 1024),
        name='attention_block',
    )(seq_len, x_in, gamma_attn, b_qkv, k_cache.reshape(flat), v_cache.reshape(flat), w_qkv)
    return ctx, k_out.reshape(k_cache.shape), v_out.reshape(v_cache.shape)


FT = 1024
HT = 256


PT = 512
PSLOTS = 6
AHEAD = 2
HOP = 3
FAR = 3
SHIFT = 2.0 ** 64


def mlp_kernel(ctx_in, x_in, gm_in, wp, wi, wo, out_ref,
               gs, rows_all, rs_all, wib, wob, gbuf, facc, acc, topart, frompart, outbox,
               from_l, from_r, mid_l, mid_r,
               psem, wsem, osem, gsend, grecv, psend, precv, bsend, brecv):
    me = lax.axis_index('grp')
    chips = lax.axis_size('grp') // 2
    chip, core = me // 2, me % 2
    right = lax.rem(chip + 1, chips) * 2 + core
    left = lax.rem(chip + chips - 1, chips) * 2 + core
    partner = chip * 2 + 1 - core
    r = x_in.shape[0]
    s, g, br = r // 2, 2 * r, 4 * r
    hidden = wo.shape[0]
    full = hidden // HT
    rest = hidden - full * HT
    hpad = wob.shape[0]
    tiles = wo.shape[1] // FT

    def w_copy(j):
        part = pl.ds(pl.multiple_of(j * HT, HT), HT)
        return pltpu.make_async_copy(wi.at[:, part], wib.at[:, part], wsem.at[j])

    last_in = pltpu.make_async_copy(wi.at[:, pl.ds(full * HT, rest)], wib.at[:, pl.ds(full * HT, rest)], wsem.at[full])
    o_copy = pltpu.make_async_copy(wo, wob.at[pl.ds(0, hidden)], osem)
    p_tiles = wp.shape[1] // PT
    depth = wp.shape[0] // PT

    def p_part(t, k):
        slot = t % PSLOTS
        buf, row = (wob, slot * PT) if slot < PSLOTS // 2 else (wib.at[1], (slot - PSLOTS // 2) * PT)
        return buf.at[pl.ds(row, PT), pl.ds(k * PT, PT)]

    def p_copy(t, k):
        return pltpu.make_async_copy(wp.at[pl.ds(k * PT, PT), pl.ds(t * PT, PT)], p_part(t, k), psem.at[t % PSLOTS, k])

    for t in range(AHEAD):
        for k in range(depth):
            p_copy(t, k).start()
    gs[...] = gm_in[...].astype(F32)[None, :] * (1.0 / SHIFT)

    barrier = pltpu.get_barrier_semaphore()
    for dev in (right, left, partner):
        pl.semaphore_signal(barrier, inc=1, device_id={'grp': dev}, device_id_type=pl.DeviceIdType.MESH)
    pl.semaphore_wait(barrier, 3)

    def remote(src, dst, send, recv, dev):
        return pltpu.make_async_remote_copy(src_ref=src, dst_ref=dst, send_sem=send, recv_sem=recv,
                                            device_id={'grp': dev}, device_id_type=pl.DeviceIdType.MESH)

    def gather(n, src, dst, count, dev):
        def at(c):
            def view(first):
                if c == p_tiles:
                    return rs_all.at[pl.ds(first, count)]
                return rows_all.at[pl.ds(first, count), pl.ds(c * PT, PT)]
            return remote(view(src), view(dst), gsend.at[n, c], grecv.at[n, c], dev)
        return at

    to_r0 = gather(0, br, r, s, right)
    to_l1 = gather(1, br + s, r + s, s, left)
    to_r1 = gather(2, br + s, br + r, s, right)
    to_l0 = gather(3, br, br + r + s, s, left)
    to_p = gather(4, br, br + g, r, partner)
    on_r = gather(5, r, 0, s, right)
    on_l = gather(6, r + s, s, s, left)
    p_l0 = gather(7, r, g + r, s, partner)
    p_r1 = gather(8, r + s, g + r + s, s, partner)
    p_l1 = gather(9, br + r, br + g + r, s, partner)
    p_r0 = gather(10, br + r + s, br + g + r + s, s, partner)
    p_o0 = gather(11, 0, g, s, partner)
    p_o1 = gather(12, s, g + s, s, partner)
    gathers = [to_r0, to_l1, to_r1, to_l0, to_p, on_r, on_l, p_l0, p_r1, p_l1, p_r0, p_o0, p_o1]

    def pass_first(c):
        to_r0(c).wait_recv()
        on_r(c).start()
        p_l0(c).start()
        to_l1(c).wait_recv()
        on_l(c).start()
        p_r1(c).start()

    def pass_second(c):
        to_r1(c).wait_recv()
        p_l1(c).start()
        to_l0(c).wait_recv()
        p_r0(c).start()

    def pass_far(c):
        on_r(c).wait_recv()
        p_o0(c).start()
        on_l(c).wait_recv()
        p_o1(c).start()

    if hpad > hidden:
        wib[:, hidden:, :] = jnp.zeros((2, hpad - hidden, wib.shape[2]), BF16)
        wob[hidden:, :] = jnp.zeros((hpad - hidden, wob.shape[1]), BF16)

    square = jnp.zeros((r, HEAD_DIM), F32)
    for t in range(p_tiles):
        part = slice(t * PT, (t + 1) * PT)
        out = None
        for k in range(depth):
            p_copy(t, k).wait()
        if t + AHEAD < p_tiles:
            for k in range(depth):
                p_copy(t + AHEAD, k).start()
        for k in range(depth):
            term = jnp.dot(ctx_in[:, k * PT:(k + 1) * PT], p_part(t, k)[...], preferred_element_type=F32)
            out = term if out is None else out + term
        hid = x_in[:, part].astype(F32) + out
        acc[:, part] = hid
        rows_all[br:br + r, part] = (hid * gs[:, part]).astype(BF16)
        for copy in (to_r0, to_l1, to_p):
            copy(t).start()
        if t < HOP:
            to_r1(t).start()
            to_l0(t).start()
        for k in range(PT // HEAD_DIM):
            lanes = hid[:, k * HEAD_DIM:(k + 1) * HEAD_DIM]
            square = square + lanes * lanes
        if t == p_tiles - 2:
            w_copy(0).start()
        if t >= HOP:
            pass_first(t - HOP)
            if t - HOP < HOP:
                pass_second(t - HOP)
        if t >= HOP + FAR:
            pass_far(t - HOP - FAR)
    loads = [w_copy(j) for j in range(1, full)] + ([last_in] if rest else []) + [o_copy]
    mean_sq = jnp.sum(square, axis=-1, keepdims=True) / wp.shape[1]
    rs_all[br:br + r, :] = jnp.broadcast_to(lax.rsqrt(mean_sq + EPS) * SHIFT, (r, HEAD_DIM))
    for copy in (to_r0, to_l1, to_p):
        copy(p_tiles).start()
    for c in range(p_tiles - HOP, p_tiles + 1):
        for copy in loads[:2]:
            copy.start()
        loads = loads[2:]
        pass_first(c)
        pass_far(c - FAR)
    for copy in loads:
        copy.start()
    for c in range(HOP, p_tiles + 1):
        to_r1(c).start()
        to_l0(c).start()
    for c in range(p_tiles - FAR + 1, p_tiles + 1):
        pass_far(c)
    for c in range(p_tiles + 1):
        for copy in (p_l0, p_r1, p_o0, p_o1):
            copy(c).wait_recv()

    def gate_tile(blk, j):
        part = pl.ds(pl.multiple_of(j * HT, HT), HT)
        x = rows_all[pl.ds(blk * br, br)]
        dims = (((1,), (1,)), ((), ()))
        gate = lax.dot_general(x, wib[0, part, :], dims, preferred_element_type=F32)
        up = lax.dot_general(x, wib[1, part, :], dims, preferred_element_type=F32)
        scale = rs_all[pl.ds(blk * br, br), 0:1]
        gate = jnp.where(scale > 0.0, gate * scale, 0.0)
        up = jnp.where(scale > 0.0, up * scale, 0.0)
        gbuf[:, part] = (jax.nn.silu(gate) * up).astype(BF16)

    def cols(t):
        return slice(t * FT, (t + 1) * FT)

    def to_partner(blk, t):
        return remote(topart.at[t], frompart.at[blk, t], psend.at[blk, t], precv.at[blk, t], partner)

    def out_copy(kind, t):
        dst = (from_r.at[0, t], from_l.at[1, t], mid_l.at[t], mid_r.at[t], from_l.at[0, t], from_r.at[1, t])[kind]
        dev = (left, right, right, left, right, left)[kind]
        return remote(outbox.at[kind, t], dst, bsend.at[kind, t], brecv.at[kind, t], dev)

    def post(kind, t, vals):
        outbox[kind, t] = vals.astype(BF16)
        out_copy(kind, t).start()

    def down_tile(blk, t):
        f = jnp.dot(gbuf[...], wob[:, cols(t)], preferred_element_type=F32)
        if blk == 1:
            to_partner(0, t).wait_send()
        topart[t] = f[g:].astype(BF16)
        to_partner(blk, t).start()
        facc[t % 3] = f[:g]

    def finish(blk, t):
        to_partner(blk, t).wait_recv()
        total = facc[t % 3] + frompart[blk, t].astype(F32)
        if blk == 0:
            post(2, t, total[:s])
            post(3, t, total[s:r])
            post(0, t, total[r:r + s])
            post(1, t, total[r + s:])
        else:
            acc[:, cols(t)] += total[:r]
            out_copy(2, t).wait_recv()
            post(4, t, total[r + s:] + mid_l[t].astype(F32))
            out_copy(3, t).wait_recv()
            post(5, t, total[r:r + s] + mid_r[t].astype(F32))

    def first_step(j, carry):
        w_copy(j).wait()
        gate_tile(0, j)
        return carry

    def second_step(j, carry):
        gate_tile(1, j)
        return carry

    lax.fori_loop(0, full, first_step, 0)
    if rest:
        last_in.wait()
        gate_tile(0, full)
    for c in range(min(HOP, p_tiles - HOP), p_tiles + 1):
        pass_second(c)
    o_copy.wait()
    for t in range(tiles):
        down_tile(0, t)
        if t >= 2:
            finish(0, t - 2)
    finish(0, tiles - 2)
    for c in range(p_tiles + 1):
        for copy in (to_p, p_l1, p_r0):
            copy(c).wait_recv()
    gate_tile(1, 0)
    finish(0, tiles - 1)
    lax.fori_loop(1, hpad // HT, second_step, 0)
    for t in range(tiles):
        down_tile(1, t)
        if t:
            finish(1, t - 1)
    finish(1, tiles - 1)
    for t in range(tiles):
        for kind in (0, 1, 4, 5):
            out_copy(kind, t).wait_recv()
        for half in range(2):
            part = slice(half * s, (half + 1) * s)
            total = acc[part, cols(t)] + (from_l[half, t].astype(F32) + from_r[half, t].astype(F32))
            out_ref[part, cols(t)] = total.astype(BF16)
    for copy in gathers:
        for c in range(p_tiles + 1):
            copy(c).wait_send()
    for t in range(tiles):
        to_partner(1, t).wait_send()
        for kind in range(6):
            out_copy(kind, t).wait_send()


def mlp_block(ctx, x_in, gamma_mlp, w_proj, w_in, w_out):
    rows, width = x_in.shape
    hidden = w_out.shape[0]
    hpad = -(-hidden // HT) * HT
    tiles = width // FT
    half, group, block = rows // 2, 2 * rows, 4 * rows
    hbm = pl.BlockSpec(memory_space=pl.ANY)
    vmem = pl.BlockSpec(memory_space=pltpu.VMEM)
    dma = pltpu.SemaphoreType.DMA
    return pl.pallas_call(
        mlp_kernel,
        out_shape=pltpu.VMEM((rows, width), BF16),
        in_specs=[vmem] * 3 + [hbm] * 3,
        out_specs=vmem,
        scratch_shapes=[
            pltpu.VMEM((1, width), F32),
            pltpu.VMEM((2 * block, width), BF16),
            pltpu.VMEM((2 * block, HEAD_DIM), F32),
            pltpu.VMEM((2, hpad, width), BF16),
            pltpu.VMEM((hpad, width), BF16),
            pltpu.VMEM((block, hpad), BF16),
            pltpu.VMEM((3, group, FT), F32),
            pltpu.VMEM((rows, width), F32),
            pltpu.VMEM((tiles, group, FT), BF16),
            pltpu.VMEM((2, tiles, group, FT), BF16),
            pltpu.VMEM((6, tiles, half, FT), BF16),
            pltpu.VMEM((2, tiles, half, FT), BF16),
            pltpu.VMEM((2, tiles, half, FT), BF16),
            pltpu.VMEM((tiles, half, FT), BF16),
            pltpu.VMEM((tiles, half, FT), BF16),
            dma((PSLOTS, w_proj.shape[0] // PT)), dma((hpad // HT,)), dma, dma((13, width // PT + 1)), dma((13, width // PT + 1)),
            dma((2, tiles)), dma((2, tiles)), dma((6, tiles)), dma((6, tiles)),
        ],
        compiler_params=pltpu.CompilerParams(vmem_limit_bytes=60 * 1024 * 1024, collective_id=0, has_side_effects=True),
        name='mlp_block',
    )(ctx, x_in, gamma_mlp, w_proj, w_in, w_out)


def solution(mesh):
    row_spec = P(('rep', 'grp'))
    repl_spec = P()

    def local_layer(x_in, seq_len, k_cache, v_cache, gamma_attn, w_qkv, b_qkv, w_proj, gamma_mlp, w_in, w_out):
        ctx, k_out, v_out = attention_block(x_in, seq_len, k_cache, v_cache, gamma_attn, w_qkv, b_qkv)
        ctx = pltpu.with_memory_space_constraint(ctx, pltpu.VMEM)
        layer_out = mlp_block(ctx, x_in, gamma_mlp, w_proj, w_in, w_out)
        return layer_out, k_out, v_out

    return jax.shard_map(local_layer, mesh=mesh,
                         in_specs=(row_spec, row_spec, row_spec, row_spec, repl_spec, repl_spec, repl_spec,
                                   repl_spec, repl_spec, P(None, 'grp', None), P('grp', None)),
                         out_specs=(row_spec, row_spec, row_spec), check_vma=False)
```
